128 devices in a mesh: gx: 32 (over x, z, core), gy: 4 (over y).
Axes of the slice: x: 4, y: 4, z: 4, core: 2. Of those that a mesh axis runs over, the one named last changes fastest.
Arguments:
- velocity: float32 [3, 256, 256, 256], P(None, 'gx', 'gy'), may hold values from -10 to 10
Outputs:
- coefficient: float32 [256], P('gy')
- viscosity: float32 [256, 256, 256], P('gx', 'gy')
The draws below stay inside these ranges and needn't reach their ends.
All inputs are finite; a program needn't handle non-finite values.
Results may differ from the reference program's by a relative error of at most 0.00002.
Values sent between devices are 32-bit elements; how exact they have to be, the bound alone decides.
A program may use at most 64 MiB of HBM per device.

```python
import jax
import jax.numpy as jnp
from jax import lax

NZ = 256
NX = 256
NY = 256


def draw_velocity(key, part):
    noise_key = jax.random.fold_in(key, 0)
    stream_pos = jnp.arange(NX, dtype=jnp.float32) / NX
    wall_pos = (jnp.arange(NY, dtype=jnp.float32) + 0.5) / NY
    amplitude = (0.5 + stream_pos)[:, None, None] * (0.5 + wall_pos)[None, :, None]
    fluctuation = jax.random.normal(noise_key, (3, NX, NY, NZ), jnp.float32)
    mean_flow = 6.0 * wall_pos * (1.0 - wall_pos)
    mean_field = jnp.stack([mean_flow, 0.0 * mean_flow, 0.0 * mean_flow])
    velocity_field = amplitude[None] * fluctuation + mean_field[:, None, :, None]
    return jnp.clip(velocity_field, -10.0, 10.0)


def setup_inputs(seed: int = 0) -> dict:
    arg_keys = jax.random.split(jax.random.key(seed), 2)
    velocity = draw_velocity(jax.random.fold_in(arg_keys[1], 71), 0)
    return {"velocity": velocity}


step_stream = 2.0
step_wall = 0.5
step_span = 1.0
clip_high = 0.1
weights = (1.0, 1.0, 1.0, 2.0, 2.0, 2.0)
index_pairs = ((0, 0), (1, 1), (2, 2), (0, 1), (0, 2), (1, 2))

def strain_inner(padded):
    grad_stream = (padded[:, 2:, 1:-1] - padded[:, :-2, 1:-1]) * (0.5 / step_stream)
    grad_wall = (padded[:, 1:-1, 2:] - padded[:, 1:-1, :-2]) * (0.5 / step_wall)
    centre = padded[:, 1:-1, 1:-1]
    grad_span = (jnp.roll(centre, -1, 3) - jnp.roll(centre, 1, 3)) * (0.5 / step_span)
    gradients = (grad_stream, grad_wall, grad_span)
    return jnp.stack([0.5 * (gradients[second][first] + gradients[first][second]) for first, second in index_pairs])

def weight_column():
    return jnp.asarray(weights, jnp.float32).reshape(6, 1, 1, 1)

def magnitude(strain):
    return jnp.sqrt(2.0 * lax.optimization_barrier(jnp.sum(weight_column() * strain * strain, axis=0)))

def test_filter(field):
    smoothed = 0.25 * field[:, :-2] + 0.5 * field[:, 1:-1] + 0.25 * field[:, 2:]
    return 0.25 * jnp.roll(smoothed, 1, 3) + 0.5 * smoothed + 0.25 * jnp.roll(smoothed, -1, 3)

def plane_sums(velocity_pad, stress_pad, filtered_pad):
    strain_hat = strain_inner(filtered_pad)
    magnitude_hat = magnitude(strain_hat)
    row_values = velocity_pad[:, :, 1:-1]
    products = jnp.stack([row_values[first] * row_values[second] for first, second in index_pairs])
    product_hat = test_filter(products)
    centre = filtered_pad[:, 1:-1, 1:-1]
    leonard = product_hat - jnp.stack([centre[first] * centre[second] for first, second in index_pairs])
    trace_third = (leonard[0] + leonard[1] + leonard[2]) / 3.0
    leonard = jnp.concatenate([leonard[:3] - trace_third[None], leonard[3:]])
    model_tensor = 2.0 * (test_filter(stress_pad) - 4.0 * magnitude_hat[None] * strain_hat)
    numerator = lax.optimization_barrier(jnp.sum(weight_column() * leonard * model_tensor, axis=(0, 1, 3)))
    denominator = lax.optimization_barrier(jnp.sum(weight_column() * model_tensor * model_tensor, axis=(0, 1, 3)))
    return (numerator, denominator)

def wrap_stream(field):
    return jnp.concatenate([field[:, -1:], field, field[:, :1]], axis=1)

def pad_walls(field):
    return jnp.pad(field, ((0, 0), (0, 0), (1, 1), (0, 0)))

def reference(velocity):
    velocity_pad = pad_walls(wrap_stream(velocity))
    strain = strain_inner(velocity_pad)
    strength = magnitude(strain)
    stress = strength[None] * strain
    filtered = test_filter(velocity_pad[:, :, 1:-1])
    filtered_pad = pad_walls(wrap_stream(filtered))
    stress_pad = wrap_stream(stress)
    numerator, denominator = plane_sums(velocity_pad, stress_pad, filtered_pad)
    raw_profile = jnp.clip(numerator / denominator, 0.0, clip_high)
    rim_values = jnp.concatenate([raw_profile[:1], raw_profile, raw_profile[-1:]])
    smooth = 0.25 * rim_values[:-2] + 0.5 * raw_profile + 0.25 * rim_values[2:]
    return (smooth, smooth[None, :, None] * strength)
```

```python
import functools

import jax
import jax.numpy as jnp
from jax import lax
from jax.experimental import pallas as pl
from jax.experimental.pallas import tpu as pltpu
from jax.sharding import PartitionSpec as P

F32 = jnp.float32
MESH = pl.DeviceIdType.MESH
XL = 8
YL = 64
ZL = 256
HALF = 128
CHUNKS = 4
CHUNK = YL // CHUNKS
clip_high = 0.1


def next_odd(a):
    return pltpu.roll(a, HALF - 1, 1)


def prev_even(a):
    return pltpu.roll(a, 1, 1)


def span_diff(even, odd):
    return odd - prev_even(odd), next_odd(even) - even


def span_sum(even, odd):
    pair_even = even + odd
    pair_odd = odd + next_odd(even)
    return pair_even + prev_even(pair_odd), pair_even + pair_odd


def gradients(ref, row, start, lead):
    stream = [[None] * 2 for _ in range(3)]
    wall = [[None] * 2 for _ in range(3)]
    span = [None] * 3
    middle = [[None] * 2 for _ in range(3)]
    sides = [[None] * 2 for _ in range(3)]
    for c in range(3):
        for h in range(2):
            above = ref[row + 1, c, h, start : start + 8, :]
            below = ref[row - 1, c, h, start : start + 8, :]
            stream[c][h] = above - below
            sides[c][h] = above + below if lead else None
            wall[c][h] = (
                ref[row, c, h, start + 1 : start + 9, :] - ref[row, c, h, start - 1 : start + 7, :]
            )
            middle[c][h] = ref[row, c, h, start : start + 8, :]
        span[c] = span_diff(middle[c][0], middle[c][1])
    return stream, wall, span, middle, sides


def tensor(stream, wall, span, h):
    d0, d1, d2 = stream[0][h], wall[1][h], span[2][h]
    t01 = wall[0][h] + 0.25 * stream[1][h]
    t02 = span[0][h] + 0.5 * stream[2][h]
    t12 = span[1][h] + 2.0 * wall[2][h]
    square = t01 * t01 + 0.25 * (0.5 * (d0 * d0) + t02 * t02 + t12 * t12)
    square = square + (2.0 * (d1 * d1) + 0.5 * (d2 * d2))
    return (d0, d1, d2, t01, t02, t12), jnp.sqrt(square)


def strain_unit(w, st, vf, sr, xi, k):
    r = 6 + 8 * k
    stream, wall, span, middle, sides = gradients(w, xi + 1, r, True)
    for h in range(2):
        parts, mag = tensor(stream, wall, span, h)
        quarter, half = 0.25 * mag, 0.5 * mag
        factors = (quarter, mag, half, half, quarter, quarter)
        for p in range(6):
            st[xi, p, h, 8 * k : 8 * k + 8, :] = factors[p] * parts[p]
        sr[xi, h, 8 * k : 8 * k + 8, :] = mag
    for c in range(3):
        smooth = [sides[c][h] + (middle[c][h] + middle[c][h]) for h in range(2)]
        both = span_sum(smooth[0], smooth[1])
        for h in range(2):
            vf[xi, c, h, 8 + 8 * k : 16 + 8 * k, :] = 0.25 * both[h]


def sums_unit(w, st, vf, acc, xo, k):
    r = 6 + 8 * k
    j = 8 * k
    stream, wall, span, middle, _ = gradients(vf, xo + 1, 8 + j, False)
    model = [[None] * 6 for _ in range(2)]
    leonard = [[None] * 6 for _ in range(2)]
    for p in range(6):
        line = []
        for h in range(2):
            mid = st[xo + 1, p, h, j : j + 8, :]
            line.append(
                st[xo, p, h, j : j + 8, :] + st[xo + 2, p, h, j : j + 8, :] + (mid + mid)
            )
        both = span_sum(line[0], line[1])
        for h in range(2):
            model[h][p] = both[h]
    for h in range(2):
        parts, mag = tensor(stream, wall, span, h)
        twice, four = 2.0 * mag, 4.0 * mag
        factors = (mag, four, twice, twice, mag, mag)
        for p in range(6):
            model[h][p] = model[h][p] - factors[p] * parts[p]
    rows = [
        [[w[xo + 1 + i, c, h, r : r + 8, :] for h in range(2)] for c in range(3)] for i in range(3)
    ]
    for p, (a, b) in enumerate(((0, 0), (1, 1), (2, 2), (0, 1), (0, 2), (1, 2))):
        line = []
        for h in range(2):
            mid = rows[1][a][h] * rows[1][b][h]
            line.append(
                rows[0][a][h] * rows[0][b][h] + rows[2][a][h] * rows[2][b][h] + (mid + mid)
            )
        both = span_sum(line[0], line[1])
        for h in range(2):
            leonard[h][p] = both[h] - middle[a][h] * middle[b][h]
    num = den = None
    for h in range(2):
        lo, mo = leonard[h], model[h]
        third = (lo[0] + lo[1] + lo[2]) * (1.0 / 3.0)
        n_diag = (lo[0] - third) * mo[0] + (lo[1] - third) * mo[1] + (lo[2] - third) * mo[2]
        n_off = lo[3] * mo[3] + lo[4] * mo[4] + lo[5] * mo[5]
        d_diag = mo[0] * mo[0] + mo[1] * mo[1] + mo[2] * mo[2]
        d_off = mo[3] * mo[3] + mo[4] * mo[4] + mo[5] * mo[5]
        n = n_diag + (n_off + n_off)
        d = d_diag + (d_off + d_off)
        num = n if num is None else num + n
        den = d if den is None else den + d
    acc[0, j : j + 8, :] += num
    acc[1, j : j + 8, :] += den


def over_rows(base, count, body):
    def step(i, carry):
        body(base + i)
        return carry

    lax.fori_loop(0, count, step, 0)


def main_kernel(
    nx, ny,
    vel, strength, cexp, crow,
    nat, w, st, vf, sr, acc, msg, gath,
    in_sem, slow_send, slow_recv, fast_send, fast_recv, wall_send, wall_recv,
    corner_send, corner_recv, sum_send, sum_recv,
):
    mx = lax.axis_index("gx")
    my = lax.axis_index("gy")
    core = lax.rem(mx, 2)
    right = lax.rem(mx + 1, nx)
    left = lax.rem(mx + nx - 1, nx)
    slow = core * right + (1 - core) * left
    fast = core * left + (1 - core) * right
    has_low = my > 0
    has_high = my < ny - 1

    barrier = pltpu.get_barrier_semaphore()
    for p in range(1, nx):
        pl.semaphore_signal(
            barrier, inc=1, device_id=(lax.rem(mx + p, nx), my), device_id_type=MESH
        )

    @pl.when(has_low)
    def _():
        pl.semaphore_signal(barrier, inc=1, device_id=(mx, my - 1), device_id_type=MESH)

    @pl.when(has_high)
    def _():
        pl.semaphore_signal(barrier, inc=1, device_id=(mx, my + 1), device_id_type=MESH)

    loads = [
        pltpu.make_async_copy(
            vel.at[:, 2 * g : 2 * g + 2], nat.at[:, 2 * g : 2 * g + 2], in_sem.at[g]
        )
        for g in range(4)
    ]
    for load in loads:
        load.start()

    def clear(first, count):
        def body(x):
            for c in range(3):
                for h in range(2):
                    w[x, c, h, first : first + count, :] = jnp.zeros((count, HALF), F32)

        return lambda: over_rows(0, 12, body)

    clear(0, 6)()
    clear(74, 6)()
    pl.when(jnp.logical_not(has_low))(clear(6, 2))
    pl.when(jnp.logical_not(has_high))(clear(72, 2))
    acc[...] = jnp.zeros_like(acc)

    lane = lax.broadcasted_iota(jnp.int32, (8, HALF), 1)
    sub = lax.broadcasted_iota(jnp.int32, (8, HALF), 0)
    low_lane = lane < 64
    pick_left = lax.rem(lane, 64) * 2 + lax.div(lane, 64)
    pick_right = lax.rem(lane, 64) * 2 + (1 - lax.div(lane, 64))

    def split(x):
        for c in range(3):
            for m in range(8):
                a = nat[c, x, 8 * m : 8 * m + 8, 0:128]
                b = nat[c, x, 8 * m : 8 * m + 8, 128:256]
                a = jnp.take_along_axis(a, pick_left, axis=1)
                b = jnp.take_along_axis(b, pick_right, axis=1)
                w[x + 2, c, 0, 8 + 8 * m : 16 + 8 * m, :] = jnp.where(low_lane, a, b)
                w[x + 2, c, 1, 8 + 8 * m : 16 + 8 * m, :] = pltpu.roll(
                    jnp.where(low_lane, b, a), 64, 1
                )

    for g in range(4):
        loads[g].wait()
        over_rows(2 * g, 2, split)

    pl.semaphore_wait(
        barrier, nx - 1 + has_low.astype(jnp.int32) + has_high.astype(jnp.int32)
    )

    def edge(src, dst, rows_from, rows_to, count, sems, to):
        return pltpu.make_async_remote_copy(
            src_ref=w.at[pl.ds(src[0], src[1]), :, :, rows_from : rows_from + count, :],
            dst_ref=w.at[pl.ds(dst[0], dst[1]), :, :, rows_to : rows_to + count, :],
            send_sem=sems[0],
            recv_sem=sems[1],
            device_id=to,
            device_id_type=MESH,
        )

    slow_src, slow_dst = 2 + 6 * core, 10 - 10 * core
    fast_src, fast_dst = 8 - 6 * core, 10 * core
    slow_copies = [
        edge(
            (slow_src, 2), (slow_dst, 2), 8 + CHUNK * c, 8 + CHUNK * c, CHUNK,
            (slow_send.at[c], slow_recv.at[c]), (slow, my),
        )
        for c in range(CHUNKS)
    ]
    fast_copy = edge((fast_src, 2), (fast_dst, 2), 8, 8, YL, (fast_send, fast_recv), (fast, my))
    to_low = edge((2, 8), (2, 8), 8, 72, 2, (wall_send.at[0], wall_recv.at[0]), (mx, my - 1))
    to_high = edge((2, 8), (2, 8), 70, 6, 2, (wall_send.at[1], wall_recv.at[1]), (mx, my + 1))
    slow_copies[0].start()
    pl.when(has_low)(to_low.start)
    pl.when(has_high)(to_high.start)
    fast_copy.start()
    for c in range(1, CHUNKS):
        slow_copies[c].start()

    def strains(ks):
        def body(xi):
            for k in ks:
                strain_unit(w, st, vf, sr, xi, k)

        return body

    def sums(ks):
        def body(xo):
            for k in ks:
                sums_unit(w, st, vf, acc, xo, k)

        return body

    fast_first = 8 - 8 * core
    near_first = 2 - 2 * core
    over_rows(2, 6, strains(range(1, 8)))
    fast_copy.wait_recv()
    over_rows(fast_first, 2, strains(range(1, 8)))
    over_rows(near_first, 6, sums(range(2, 7)))

    corner_slow_low = edge(
        (slow_src, 2), (slow_dst, 2), 6, 6, 2, (corner_send.at[0], corner_recv.at[0]), (slow, my)
    )
    corner_slow_high = edge(
        (slow_src, 2), (slow_dst, 2), 72, 72, 2, (corner_send.at[1], corner_recv.at[1]), (slow, my)
    )
    corner_fast_low = edge(
        (fast_src, 2), (fast_dst, 2), 6, 6, 2, (corner_send.at[2], corner_recv.at[2]), (fast, my)
    )
    corner_fast_high = edge(
        (fast_src, 2), (fast_dst, 2), 72, 72, 2, (corner_send.at[3], corner_recv.at[3]), (fast, my)
    )

    @pl.when(has_low)
    def _():
        to_high.wait_recv()
        corner_slow_low.start()
        corner_fast_low.start()

    @pl.when(has_high)
    def _():
        to_low.wait_recv()
        corner_slow_high.start()
        corner_fast_high.start()

    over_rows(2, 6, strains((0, 8)))
    pl.when(has_low)(corner_fast_low.wait_recv)
    pl.when(has_high)(corner_fast_high.wait_recv)
    over_rows(fast_first, 2, strains((0, 8)))
    over_rows(near_first, 6, sums((0, 1, 7, 8)))

    slow_first = 8 * core
    far_first = 6 * core
    groups = (((0, 1), (0,)), ((2, 3), (1, 2)), ((4, 5), (3, 4)), ((6, 7, 8), (5, 6, 7, 8)))
    for c in range(CHUNKS):
        slow_copies[c].wait_recv()
        if c == 0:
            pl.when(has_low)(corner_slow_low.wait_recv)
        if c == CHUNKS - 1:
            pl.when(has_high)(corner_slow_high.wait_recv)
        over_rows(slow_first, 2, strains(groups[c][0]))
        over_rows(far_first, 2, sums(groups[c][1]))

    packs = []
    for q in range(2):
        table = jnp.zeros((8, HALF), F32)
        for k in range(9):
            column = jnp.sum(acc[q, 8 * k : 8 * k + 8, :], axis=1, keepdims=True)
            table = jnp.where(lane == k, column, table)
        spread = pltpu.roll(table, 0, 1, stride=16, stride_axis=0)
        packs.append(jnp.sum(spread, axis=0, keepdims=True))
    for q in range(2):
        msg[q : q + 1, :] = packs[q]
        gath[mx, q : q + 1, :] = packs[q]

    def gather_copy(to):
        return pltpu.make_async_remote_copy(
            src_ref=msg,
            dst_ref=gath.at[mx],
            send_sem=sum_send,
            recv_sem=sum_recv,
            device_id=(to, my),
            device_id_type=MESH,
        )

    for p in range(1, nx):
        gather_copy(lax.rem(mx + p, nx)).start()

    even_lane = lax.rem(lane, 2) == 0
    pick_low = lax.div(lane, 2)
    pick_high = pick_low + 64

    def join(x):
        for m in range(8):
            even = sr[x + 1, 0, 8 * m + 2 : 8 * m + 10, :]
            odd = sr[x + 1, 1, 8 * m + 2 : 8 * m + 10, :]
            for side, pick in enumerate((pick_low, pick_high)):
                strength[x, 8 * m : 8 * m + 8, 128 * side : 128 * side + 128] = jnp.where(
                    even_lane,
                    jnp.take_along_axis(even, pick, axis=1),
                    jnp.take_along_axis(odd, pick, axis=1),
                )

    over_rows(0, XL, join)

    everyone = pltpu.make_async_remote_copy(
        src_ref=gath.at[0 : nx - 1],
        dst_ref=gath.at[0 : nx - 1],
        send_sem=sum_send,
        recv_sem=sum_recv,
        device_id=(right, my),
        device_id_type=MESH,
    )
    everyone.wait_recv()
    terms = [gath[i] for i in range(nx)]
    while len(terms) > 1:
        terms = [a + b for a, b in zip(terms[::2], terms[1::2])]
    total = terms[0]
    raw = jnp.clip(0.5 * (total[0:1, :] / total[1:2, :]), 0.0, clip_high)
    raw = jnp.broadcast_to(raw, (8, HALF))
    below = jnp.where(lane < 16, pltpu.roll(raw, 17, 1), pltpu.roll(raw, 16, 1))
    above = jnp.where(lane >= 112, pltpu.roll(raw, 111, 1), pltpu.roll(raw, 112, 1))
    below = jnp.where(jnp.logical_and(lane == 32, jnp.logical_not(has_low)), raw, below)
    above = jnp.where(jnp.logical_and(lane == 24, jnp.logical_not(has_high)), raw, above)
    smooth = 0.25 * below + 0.5 * raw + 0.25 * above
    row = lane + 2
    crow[...] = jnp.take_along_axis(
        smooth, lax.rem(16 * lax.rem(row, 8) + lax.div(row, 8), HALF), axis=1
    )
    row = 8 * lane + sub + 2
    cexp[...] = jnp.take_along_axis(
        smooth, lax.rem(16 * lax.rem(row, 8) + lax.div(row, 8), HALF), axis=1
    )

    for copy in slow_copies:
        copy.wait_send()
    fast_copy.wait_send()

    @pl.when(has_low)
    def _():
        to_low.wait_send()
        corner_slow_low.wait_send()
        corner_fast_low.wait_send()

    @pl.when(has_high)
    def _():
        to_high.wait_send()
        corner_slow_high.wait_send()
        corner_fast_high.wait_send()

    everyone.wait_send()


def scale_kernel(strength, cexp, crow, coefficient, viscosity):
    coefficient[...] = crow[0:1, 0:YL]
    for m in range(8):
        column = cexp[:, m : m + 1]
        for x in range(XL):
            for side in range(2):
                at = (x, slice(8 * m, 8 * m + 8), slice(128 * side, 128 * side + 128))
                viscosity[at] = strength[at] * column


def local(nx, ny, velocity):
    vmem = pl.BlockSpec(memory_space=pltpu.VMEM)
    dma = pltpu.SemaphoreType.DMA
    strength, cexp, crow = pl.pallas_call(
        functools.partial(main_kernel, nx, ny),
        out_shape=(
            jax.ShapeDtypeStruct((XL, YL, ZL), F32),
            jax.ShapeDtypeStruct((8, HALF), F32),
            jax.ShapeDtypeStruct((8, HALF), F32),
        ),
        in_specs=[pl.BlockSpec(memory_space=pl.ANY)],
        out_specs=(vmem, vmem, vmem),
        scratch_shapes=[
            pltpu.VMEM((3, XL, YL, ZL), F32),
            pltpu.VMEM((12, 3, 2, 80, HALF), F32),
            pltpu.VMEM((10, 6, 2, 72, HALF), F32),
            pltpu.VMEM((10, 3, 2, 88, HALF), F32),
            pltpu.VMEM((10, 2, 72, HALF), F32),
            pltpu.VMEM((2, 72, HALF), F32),
            pltpu.VMEM((2, HALF), F32),
            pltpu.VMEM((nx, 2, HALF), F32),
            dma((4,)),
            dma((CHUNKS,)),
            dma((CHUNKS,)),
            dma,
            dma,
            dma((2,)),
            dma((2,)),
            dma((4,)),
            dma((4,)),
            dma,
            dma,
        ],
        compiler_params=pltpu.CompilerParams(collective_id=0, has_side_effects=True),
        name="germano",
    )(velocity)
    coefficient, viscosity = pl.pallas_call(
        scale_kernel,
        out_shape=(
            jax.ShapeDtypeStruct((1, YL), F32),
            jax.ShapeDtypeStruct((XL, YL, ZL), F32),
        ),
        in_specs=[vmem, vmem, vmem],
        out_specs=(vmem, vmem),
        name="scale",
    )(strength, cexp, crow)
    return coefficient.reshape(YL), viscosity


def solution(mesh):
    nx, ny = mesh.shape["gx"], mesh.shape["gy"]
    return jax.shard_map(
        functools.partial(local, nx, ny),
        mesh=mesh,
        in_specs=(P(None, "gx", "gy", None),),
        out_specs=(P("gy"), P("gx", "gy", None)),
        check_vma=False,
    )
```

```python
import functools

import jax
import jax.numpy as jnp
from jax import lax
from jax.experimental import pallas as pl
from jax.experimental.pallas import tpu as pltpu
from jax.sharding import PartitionSpec as P

F32 = jnp.float32
MESH = pl.DeviceIdType.MESH
XL = 8
YL = 64
ZL = 256
HALF = 128
CHUNKS = 4
CHUNK = YL // CHUNKS
clip_high = 0.1
TINY = 1.2e-38
PAIRS = ((0, 0), (1, 1), (2, 2), (0, 1), (0, 2), (1, 2))


def shifted(even, odd):
    return pltpu.roll(odd, 1, 1), pltpu.roll(even, HALF - 1, 1)


def span_sum(even, odd, before, after):
    pair = even + odd
    return pair + (before + even), pair + (after + odd)


def at(k):
    return slice(8 * k, 8 * k + 8)


def span_unit(w, zu, dz, zp, xi, k, products):
    r = 6 + 8 * k
    even = [w[xi, c, 0, r : r + 8, :] for c in range(3)]
    odd = [w[xi, c, 1, r : r + 8, :] for c in range(3)]
    before, after = [None] * 3, [None] * 3
    for c in range(3):
        before[c], after[c] = shifted(even[c], odd[c])
    for c in range(3):
        both = span_sum(even[c], odd[c], before[c], after[c])
        zu[xi, c, 0, at(k), :], zu[xi, c, 1, at(k), :] = both
        if products:
            dz[xi - 1, c, 0, at(k), :] = odd[c] - before[c]
            dz[xi - 1, c, 1, at(k), :] = after[c] - even[c]
    if products:
        for p, (a, b) in enumerate(PAIRS):
            both = span_sum(
                even[a] * even[b], odd[a] * odd[b], before[a] * before[b], after[a] * after[b]
            )
            zp[xi - 1, p, 0, at(k), :], zp[xi - 1, p, 1, at(k), :] = both


def tensor(stream, wall, span):
    d0, d1, d2 = stream[0], wall[1], span[2]
    t01 = wall[0] + 0.25 * stream[1]
    t02 = span[0] + 0.5 * stream[2]
    t12 = span[1] + 2.0 * wall[2]
    square = t01 * t01 + 0.25 * (0.5 * (d0 * d0) + t02 * t02 + t12 * t12)
    square = square + (2.0 * (d1 * d1) + 0.5 * (d2 * d2))
    return (d0, d1, d2, t01, t02, t12), square * lax.rsqrt(jnp.maximum(square, TINY))


def strain_unit(w, zu, dz, zs, vf, dv, sr, xi, k):
    r = 6 + 8 * k
    stress = [None] * 2
    for h in range(2):
        stream = [
            w[xi + 2, c, h, r : r + 8, :] - w[xi, c, h, r : r + 8, :] for c in range(3)
        ]
        wall = [
            w[xi + 1, c, h, r + 1 : r + 9, :] - w[xi + 1, c, h, r - 1 : r + 7, :]
            for c in range(3)
        ]
        span = [dz[xi, c, h, at(k), :] for c in range(3)]
        parts, mag = tensor(stream, wall, span)
        quarter, half = 0.25 * mag, 0.5 * mag
        factors = (quarter, mag, half, half, quarter, quarter)
        stress[h] = [factors[p] * parts[p] for p in range(6)]
        sr[xi, h, at(k), :] = mag
    for p in range(6):
        before, after = shifted(stress[0][p], stress[1][p])
        both = span_sum(stress[0][p], stress[1][p], before, after)
        zs[xi, p, 0, at(k), :], zs[xi, p, 1, at(k), :] = both
    for c in range(3):
        smooth = []
        for h in range(2):
            mid = zu[xi + 1, c, h, at(k), :]
            line = (zu[xi, c, h, at(k), :] + mid) + (zu[xi + 2, c, h, at(k), :] + mid)
            smooth.append(0.25 * line)
            vf[xi, c, h, 8 + 8 * k : 16 + 8 * k, :] = smooth[h]
        before, after = shifted(smooth[0], smooth[1])
        dv[xi, c, 0, at(k), :] = smooth[1] - before
        dv[xi, c, 1, at(k), :] = after - smooth[0]


def sums_unit(zs, zp, vf, dv, acc, xo, k):
    j = 8 + 8 * k
    num = den = None
    for h in range(2):

        def lines(ref, p):
            rows = [ref[xo + i, p, h, at(k), :] for i in range(4)]
            pair = [rows[i] + rows[i + 1] for i in range(3)]
            return pair[0] + pair[1], pair[1] + pair[2]

        stress = [lines(zs, p) for p in range(6)]
        product = [lines(zp, p) for p in range(6)]
        for i in range(2):
            xi = xo + 1 + i
            stream = [
                vf[xi + 1, c, h, j : j + 8, :] - vf[xi - 1, c, h, j : j + 8, :] for c in range(3)
            ]
            wall = [
                vf[xi, c, h, j + 1 : j + 9, :] - vf[xi, c, h, j - 1 : j + 7, :]
                for c in range(3)
            ]
            span = [dv[xi, c, h, at(k), :] for c in range(3)]
            middle = [vf[xi, c, h, j : j + 8, :] for c in range(3)]
            parts, mag = tensor(stream, wall, span)
            twice, four = 2.0 * mag, 4.0 * mag
            factors = (mag, four, twice, twice, mag, mag)
            mo = [stress[p][i] - factors[p] * parts[p] for p in range(6)]
            lo = [product[p][i] - middle[a] * middle[b] for p, (a, b) in enumerate(PAIRS)]
            third = (lo[0] + lo[1] + lo[2]) * (1.0 / 3.0)
            n_diag = (lo[0] - third) * mo[0] + (lo[1] - third) * mo[1] + (lo[2] - third) * mo[2]
            n_off = lo[3] * mo[3] + lo[4] * mo[4] + lo[5] * mo[5]
            d_diag = mo[0] * mo[0] + mo[1] * mo[1] + mo[2] * mo[2]
            d_off = mo[3] * mo[3] + mo[4] * mo[4] + mo[5] * mo[5]
            n = n_diag + (n_off + n_off)
            d = d_diag + (d_off + d_off)
            num = n if num is None else num + n
            den = d if den is None else den + d
    acc[0, at(k), :] += num
    acc[1, at(k), :] += den


def over_rows(base, count, body, each=1):
    def step(i, carry):
        for e in range(each):
            body(base + each * i + e)
        return carry

    if count == each:
        step(0, 0)
    else:
        lax.fori_loop(0, count // each, step, 0)


def main_kernel(
    nx, ny,
    vel, coefficient, viscosity,
    nat, w, zu, dz, zp, zs, vf, dv, sr, strength, acc, msg, gath,
    in_sem, slow_send, slow_recv, fast_send, fast_recv, wall_send, wall_recv,
    corner_send, corner_recv, sum_send, sum_recv,
):
    mx = lax.axis_index("gx")
    my = lax.axis_index("gy")
    core = lax.rem(mx, 2)
    right = lax.rem(mx + 1, nx)
    left = lax.rem(mx + nx - 1, nx)
    slow = core * right + (1 - core) * left
    fast = core * left + (1 - core) * right
    has_low = my > 0
    has_high = my < ny - 1

    barrier = pltpu.get_barrier_semaphore()
    for p in range(1, nx):
        pl.semaphore_signal(
            barrier, inc=1, device_id=(lax.rem(mx + p, nx), my), device_id_type=MESH
        )

    @pl.when(has_low)
    def _():
        pl.semaphore_signal(barrier, inc=1, device_id=(mx, my - 1), device_id_type=MESH)

    @pl.when(has_high)
    def _():
        pl.semaphore_signal(barrier, inc=1, device_id=(mx, my + 1), device_id_type=MESH)

    loads = [
        pltpu.make_async_copy(
            vel.at[:, 2 * g : 2 * g + 2], nat.at[:, 2 * g : 2 * g + 2], in_sem.at[g]
        )
        for g in range(4)
    ]
    for load in loads:
        load.start()

    def clear(first, count):
        def body(x):
            for c in range(3):
                for h in range(2):
                    w[x, c, h, first : first + count, :] = jnp.zeros((count, HALF), F32)

        return lambda: over_rows(0, 12, body)

    clear(0, 6)()
    clear(74, 6)()
    pl.when(jnp.logical_not(has_low))(clear(6, 2))
    pl.when(jnp.logical_not(has_high))(clear(72, 2))
    acc[...] = jnp.zeros_like(acc)

    lane = lax.broadcasted_iota(jnp.int32, (8, HALF), 1)
    sub = lax.broadcasted_iota(jnp.int32, (8, HALF), 0)
    low_lane = lane < 64
    pick_left = lax.rem(lane, 64) * 2 + lax.div(lane, 64)
    pick_right = lax.rem(lane, 64) * 2 + (1 - lax.div(lane, 64))

    def split(x):
        for c in range(3):
            for m in range(8):
                a = nat[c, x, 8 * m : 8 * m + 8, 0:128]
                b = nat[c, x, 8 * m : 8 * m + 8, 128:256]
                a = jnp.take_along_axis(a, pick_left, axis=1)
                b = jnp.take_along_axis(b, pick_right, axis=1)
                w[x + 2, c, 0, 8 + 8 * m : 16 + 8 * m, :] = jnp.where(low_lane, a, b)
                w[x + 2, c, 1, 8 + 8 * m : 16 + 8 * m, :] = pltpu.roll(
                    jnp.where(low_lane, b, a), 64, 1
                )

    for g in range(4):
        loads[g].wait()
        over_rows(2 * g, 2, split)

    pl.semaphore_wait(
        barrier, nx - 1 + has_low.astype(jnp.int32) + has_high.astype(jnp.int32)
    )

    def edge(src, dst, rows_from, rows_to, count, sems, to):
        return pltpu.make_async_remote_copy(
            src_ref=w.at[pl.ds(src[0], src[1]), :, :, rows_from : rows_from + count, :],
            dst_ref=w.at[pl.ds(dst[0], dst[1]), :, :, rows_to : rows_to + count, :],
            send_sem=sems[0],
            recv_sem=sems[1],
            device_id=to,
            device_id_type=MESH,
        )

    slow_src, slow_dst = 2 + 6 * core, 10 - 10 * core
    fast_src, fast_dst = 8 - 6 * core, 10 * core
    slow_copies = [
        edge(
            (slow_src, 2), (slow_dst, 2), 8 + CHUNK * c, 8 + CHUNK * c, CHUNK,
            (slow_send.at[c], slow_recv.at[c]), (slow, my),
        )
        for c in range(CHUNKS)
    ]
    fast_copy = edge((fast_src, 2), (fast_dst, 2), 8, 8, YL, (fast_send, fast_recv), (fast, my))
    to_low = edge((2, 8), (2, 8), 8, 72, 2, (wall_send.at[0], wall_recv.at[0]), (mx, my - 1))
    to_high = edge((2, 8), (2, 8), 70, 6, 2, (wall_send.at[1], wall_recv.at[1]), (mx, my + 1))
    slow_copies[0].start()
    pl.when(has_low)(to_low.start)
    pl.when(has_high)(to_high.start)
    fast_copy.start()
    for c in range(1, CHUNKS):
        slow_copies[c].start()

    def spans(ks, products=True):
        return lambda xi: [span_unit(w, zu, dz, zp, xi, k, products) for k in ks]

    def strains(ks):
        return lambda xi: [strain_unit(w, zu, dz, zs, vf, dv, sr, xi, k) for k in ks]

    def sums(ks):
        return lambda i: [sums_unit(zs, zp, vf, dv, acc, 2 * i, k) for k in ks]

    inner = range(1, 8)
    fast_first = 8 - 8 * core
    near_pair = 1 - core
    fast_inner, fast_outer = 10 - 9 * core, 11 - 11 * core
    slow_inner, slow_outer = 1 + 9 * core, 11 * core
    over_rows(2, 8, spans(inner))
    over_rows(2, 6, strains(inner))
    fast_copy.wait_recv()
    spans(inner)(fast_inner)
    spans(inner, False)(fast_outer)
    over_rows(fast_first, 2, strains(inner))
    over_rows(near_pair, 3, sums(range(2, 7)))

    corner_slow_low = edge(
        (slow_src, 2), (slow_dst, 2), 6, 6, 2, (corner_send.at[0], corner_recv.at[0]), (slow, my)
    )
    corner_slow_high = edge(
        (slow_src, 2), (slow_dst, 2), 72, 72, 2, (corner_send.at[1], corner_recv.at[1]), (slow, my)
    )
    corner_fast_low = edge(
        (fast_src, 2), (fast_dst, 2), 6, 6, 2, (corner_send.at[2], corner_recv.at[2]), (fast, my)
    )
    corner_fast_high = edge(
        (fast_src, 2), (fast_dst, 2), 72, 72, 2, (corner_send.at[3], corner_recv.at[3]), (fast, my)
    )

    @pl.when(has_low)
    def _():
        to_high.wait_recv()
        corner_slow_low.start()
        corner_fast_low.start()

    @pl.when(has_high)
    def _():
        to_low.wait_recv()
        corner_slow_high.start()
        corner_fast_high.start()

    over_rows(2, 8, spans((0, 8)), 4)
    over_rows(2, 6, strains((0, 8)), 3)
    pl.when(has_low)(corner_fast_low.wait_recv)
    pl.when(has_high)(corner_fast_high.wait_recv)
    spans((0, 8))(fast_inner)
    spans((0, 8), False)(fast_outer)
    over_rows(fast_first, 2, strains((0, 8)), 2)
    over_rows(near_pair, 3, sums((0, 1, 7, 8)))

    slow_first = 8 * core
    far_pair = 3 * core
    groups = (((0, 1), (0,)), ((2, 3), (1, 2)), ((4, 5), (3, 4)), ((6, 7, 8), (5, 6, 7, 8)))
    for c in range(CHUNKS):
        slow_copies[c].wait_recv()
        if c == 0:
            pl.when(has_low)(corner_slow_low.wait_recv)
        if c == CHUNKS - 1:
            pl.when(has_high)(corner_slow_high.wait_recv)
        spans(groups[c][0])(slow_inner)
        spans(groups[c][0], False)(slow_outer)
        over_rows(slow_first, 2, strains(groups[c][0]), 2)
        sums(groups[c][1])(far_pair)

    packs = []
    for q in range(2):
        table = jnp.zeros((8, HALF), F32)
        for k in range(9):
            column = jnp.sum(acc[q, 8 * k : 8 * k + 8, :], axis=1, keepdims=True)
            table = jnp.where(lane == k, column, table)
        spread = pltpu.roll(table, 0, 1, stride=16, stride_axis=0)
        packs.append(jnp.sum(spread, axis=0, keepdims=True))
    for q in range(2):
        msg[q : q + 1, :] = packs[q]
        gath[mx, q : q + 1, :] = packs[q]

    def gather_copy(to):
        return pltpu.make_async_remote_copy(
            src_ref=msg,
            dst_ref=gath.at[mx],
            send_sem=sum_send,
            recv_sem=sum_recv,
            device_id=(to, my),
            device_id_type=MESH,
        )

    for p in range(1, nx):
        gather_copy(lax.rem(mx + p, nx)).start()

    even_lane = lax.rem(lane, 2) == 0
    pick_low = lax.div(lane, 2)
    pick_high = pick_low + 64

    def join(x):
        for m in range(8):
            even = sr[x + 1, 0, 8 * m + 2 : 8 * m + 10, :]
            odd = sr[x + 1, 1, 8 * m + 2 : 8 * m + 10, :]
            for side, pick in enumerate((pick_low, pick_high)):
                strength[x, 8 * m : 8 * m + 8, 128 * side : 128 * side + 128] = jnp.where(
                    even_lane,
                    jnp.take_along_axis(even, pick, axis=1),
                    jnp.take_along_axis(odd, pick, axis=1),
                )

    over_rows(0, XL, join)

    everyone = pltpu.make_async_remote_copy(
        src_ref=gath.at[0 : nx - 1],
        dst_ref=gath.at[0 : nx - 1],
        send_sem=sum_send,
        recv_sem=sum_recv,
        device_id=(right, my),
        device_id_type=MESH,
    )
    everyone.wait_recv()
    terms = [gath[i] for i in range(nx)]
    while len(terms) > 1:
        terms = [a + b for a, b in zip(terms[::2], terms[1::2])]
    total = terms[0]
    raw = jnp.clip(0.5 * (total[0:1, :] / total[1:2, :]), 0.0, clip_high)
    raw = jnp.broadcast_to(raw, (8, HALF))
    below = jnp.where(lane < 16, pltpu.roll(raw, 17, 1), pltpu.roll(raw, 16, 1))
    above = jnp.where(lane >= 112, pltpu.roll(raw, 111, 1), pltpu.roll(raw, 112, 1))
    below = jnp.where(jnp.logical_and(lane == 32, jnp.logical_not(has_low)), raw, below)
    above = jnp.where(jnp.logical_and(lane == 24, jnp.logical_not(has_high)), raw, above)
    smooth = 0.25 * below + 0.5 * raw + 0.25 * above
    row = lane + 2
    line = jnp.take_along_axis(
        smooth, lax.rem(16 * lax.rem(row, 8) + lax.div(row, 8), HALF), axis=1
    )
    coefficient[...] = line[0:1, 0:YL]
    row = 8 * lane + sub + 2
    table = jnp.take_along_axis(
        smooth, lax.rem(16 * lax.rem(row, 8) + lax.div(row, 8), HALF), axis=1
    )
    columns = [jnp.broadcast_to(table[:, m : m + 1], (8, HALF)) for m in range(8)]

    def scale(x):
        for m in range(8):
            for side in range(2):
                part = (x, at(m), slice(HALF * side, HALF * side + HALF))
                viscosity[part] = strength[part] * columns[m]

    over_rows(0, XL, scale, 2)

    for copy in slow_copies:
        copy.wait_send()
    fast_copy.wait_send()

    @pl.when(has_low)
    def _():
        to_low.wait_send()
        corner_slow_low.wait_send()
        corner_fast_low.wait_send()

    @pl.when(has_high)
    def _():
        to_high.wait_send()
        corner_slow_high.wait_send()
        corner_fast_high.wait_send()

    everyone.wait_send()


def local(nx, ny, velocity):
    vmem = pl.BlockSpec(memory_space=pltpu.VMEM)
    dma = pltpu.SemaphoreType.DMA
    coefficient, viscosity = pl.pallas_call(
        functools.partial(main_kernel, nx, ny),
        out_shape=(
            pltpu.VMEM((1, YL), F32),
            pltpu.VMEM((XL, YL, ZL), F32),
        ),
        in_specs=[pl.BlockSpec(memory_space=pl.ANY)],
        out_specs=(vmem, vmem),
        scratch_shapes=[
            pltpu.VMEM((3, XL, YL, ZL), F32),
            pltpu.VMEM((12, 3, 2, 80, HALF), F32),
            pltpu.VMEM((12, 3, 2, 72, HALF), F32),
            pltpu.VMEM((10, 3, 2, 72, HALF), F32),
            pltpu.VMEM((10, 6, 2, 72, HALF), F32),
            pltpu.VMEM((10, 6, 2, 72, HALF), F32),
            pltpu.VMEM((10, 3, 2, 88, HALF), F32),
            pltpu.VMEM((10, 3, 2, 72, HALF), F32),
            pltpu.VMEM((10, 2, 72, HALF), F32),
            pltpu.VMEM((XL, YL, ZL), F32),
            pltpu.VMEM((2, 72, HALF), F32),
            pltpu.VMEM((2, HALF), F32),
            pltpu.VMEM((nx, 2, HALF), F32),
            dma((4,)),
            dma((CHUNKS,)),
            dma((CHUNKS,)),
            dma,
            dma,
            dma((2,)),
            dma((2,)),
            dma((4,)),
            dma((4,)),
            dma,
            dma,
        ],
        compiler_params=pltpu.CompilerParams(collective_id=0, has_side_effects=True),
        name="germano",
    )(velocity)
    return coefficient.reshape(YL), viscosity


def solution(mesh):
    nx, ny = mesh.shape["gx"], mesh.shape["gy"]
    return jax.shard_map(
        functools.partial(local, nx, ny),
        mesh=mesh,
        in_specs=(P(None, "gx", "gy", None),),
        out_specs=(P("gy"), P("gx", "gy", None)),
        check_vma=False,
    )
```

```python
import functools

import jax
import jax.numpy as jnp
from jax import lax
from jax.experimental import pallas as pl
from jax.experimental.pallas import tpu as pltpu
from jax.sharding import PartitionSpec as P

F32 = jnp.float32
BF16 = jnp.bfloat16
MESH = pl.DeviceIdType.MESH
XL = 8
YL = 64
ZL = 256
HALF = 128
CUTS = (0, 24, 48, 56, 64)
CHUNKS = len(CUTS) - 1
clip_high = 0.1
TINY = 1.2e-38
PAIRS = ((0, 0), (1, 1), (2, 2), (0, 1), (0, 2), (1, 2))


def shifted(even, odd):
    return pltpu.roll(odd, 1, 1), pltpu.roll(even, HALF - 1, 1)


def span_sum(even, odd, before, after):
    pair = even + odd
    return pair + (before + even), pair + (after + odd)


def at(k):
    return slice(8 * k, 8 * k + 8)


def span_unit(w, zu, dz, zp, xi, k, products):
    r = 6 + 8 * k
    even = [w[xi, c, 0, r : r + 8, :] for c in range(3)]
    odd = [w[xi, c, 1, r : r + 8, :] for c in range(3)]
    before, after = [None] * 3, [None] * 3
    for c in range(3):
        before[c], after[c] = shifted(even[c], odd[c])
    for c in range(3):
        both = span_sum(even[c], odd[c], before[c], after[c])
        zu[xi, c, 0, at(k), :], zu[xi, c, 1, at(k), :] = both
        if products:
            dz[xi - 1, c, 0, at(k), :] = odd[c] - before[c]
            dz[xi - 1, c, 1, at(k), :] = after[c] - even[c]
    if products:
        for p, (a, b) in enumerate(PAIRS):
            both = span_sum(
                even[a] * even[b], odd[a] * odd[b], before[a] * before[b], after[a] * after[b]
            )
            zp[xi - 1, p, 0, at(k), :], zp[xi - 1, p, 1, at(k), :] = both


def tensor(stream, wall, span):
    d0, d1, d2 = stream[0], wall[1], span[2]
    t01 = wall[0] + 0.25 * stream[1]
    t02 = span[0] + 0.5 * stream[2]
    t12 = span[1] + 2.0 * wall[2]
    square = t01 * t01 + 0.25 * (0.5 * (d0 * d0) + t02 * t02 + t12 * t12)
    square = square + (2.0 * (d1 * d1) + 0.5 * (d2 * d2))
    return (d0, d1, d2, t01, t02, t12), square * lax.rsqrt(jnp.maximum(square, TINY))


def strain_unit(w, zu, dz, zs, vf, dv, sr, xi, k):
    r = 6 + 8 * k
    stress = [None] * 2
    for h in range(2):
        stream = [
            w[xi + 2, c, h, r : r + 8, :] - w[xi, c, h, r : r + 8, :] for c in range(3)
        ]
        wall = [
            w[xi + 1, c, h, r + 1 : r + 9, :] - w[xi + 1, c, h, r - 1 : r + 7, :]
            for c in range(3)
        ]
        span = [dz[xi, c, h, at(k), :] for c in range(3)]
        parts, mag = tensor(stream, wall, span)
        quarter, half = 0.25 * mag, 0.5 * mag
        factors = (quarter, mag, half, half, quarter, quarter)
        stress[h] = [factors[p] * parts[p] for p in range(6)]
        sr[xi, h, at(k), :] = mag
    for p in range(6):
        before, after = shifted(stress[0][p], stress[1][p])
        both = span_sum(stress[0][p], stress[1][p], before, after)
        zs[xi, p, 0, at(k), :], zs[xi, p, 1, at(k), :] = both
    for c in range(3):
        smooth = []
        for h in range(2):
            mid = zu[xi + 1, c, h, at(k), :]
            line = (zu[xi, c, h, at(k), :] + mid) + (zu[xi + 2, c, h, at(k), :] + mid)
            smooth.append(0.25 * line)
            vf[xi, c, h, 8 + 8 * k : 16 + 8 * k, :] = smooth[h]
        before, after = shifted(smooth[0], smooth[1])
        dv[xi, c, 0, at(k), :] = smooth[1] - before
        dv[xi, c, 1, at(k), :] = after - smooth[0]


def sums_unit(zs, zp, vf, dv, acc, xo, k):
    j = 8 + 8 * k
    num = den = None
    for h in range(2):

        def lines(ref, p):
            rows = [ref[xo + i, p, h, at(k), :] for i in range(4)]
            pair = [rows[i] + rows[i + 1] for i in range(3)]
            return pair[0] + pair[1], pair[1] + pair[2]

        stress = [lines(zs, p) for p in range(6)]
        product = [lines(zp, p) for p in range(6)]
        for i in range(2):
            xi = xo + 1 + i
            stream = [
                vf[xi + 1, c, h, j : j + 8, :] - vf[xi - 1, c, h, j : j + 8, :] for c in range(3)
            ]
            wall = [
                vf[xi, c, h, j + 1 : j + 9, :] - vf[xi, c, h, j - 1 : j + 7, :]
                for c in range(3)
            ]
            span = [dv[xi, c, h, at(k), :] for c in range(3)]
            middle = [vf[xi, c, h, j : j + 8, :] for c in range(3)]
            parts, mag = tensor(stream, wall, span)
            twice, four = 2.0 * mag, 4.0 * mag
            factors = (mag, four, twice, twice, mag, mag)
            mo = [stress[p][i] - factors[p] * parts[p] for p in range(6)]
            lo = [product[p][i] - middle[a] * middle[b] for p, (a, b) in enumerate(PAIRS)]
            third = (lo[0] + lo[1] + lo[2]) * (1.0 / 3.0)
            n_diag = (lo[0] - third) * mo[0] + (lo[1] - third) * mo[1] + (lo[2] - third) * mo[2]
            n_off = lo[3] * mo[3] + lo[4] * mo[4] + lo[5] * mo[5]
            d_diag = mo[0] * mo[0] + mo[1] * mo[1] + mo[2] * mo[2]
            d_off = mo[3] * mo[3] + mo[4] * mo[4] + mo[5] * mo[5]
            n = n_diag + (n_off + n_off)
            d = d_diag + (d_off + d_off)
            num = n if num is None else num + n
            den = d if den is None else den + d
    acc[0, at(k), :] += num
    acc[1, at(k), :] += den


def over_rows(base, count, body, each=1):
    def step(i, carry):
        for e in range(each):
            body(base + each * i + e)
        return carry

    if count == each:
        step(0, 0)
    else:
        lax.fori_loop(0, count // each, step, 0)


def main_kernel(
    nx, ny,
    vel, coefficient, viscosity,
    nat, w, zu, dz, zp, zs, vf, dv, sr, strength, acc, msg, gath, order,
    in_sem, slow_send, slow_recv, fast_send, fast_recv, wall_send, wall_recv,
    corner_send, corner_recv, sum_send, sum_recv,
):
    mx = lax.axis_index("gx")
    my = lax.axis_index("gy")
    core = lax.rem(mx, 2)
    right = lax.rem(mx + 1, nx)
    left = lax.rem(mx + nx - 1, nx)
    slow = core * right + (1 - core) * left
    fast = core * left + (1 - core) * right
    has_low = my > 0
    has_high = my < ny - 1

    def base(q):
        return core * q + (1 - core) * (10 - q)

    def signal(sem, x, y):
        pl.semaphore_signal(sem, inc=1, device_id=(x, y), device_id_type=MESH)

    loads = []
    for g, q in enumerate((8, 6, 4, 2)):
        cells = pl.ds(base(q) - 2, 2)
        loads.append(pltpu.make_async_copy(vel.at[:, cells], nat.at[:, cells], in_sem.at[g]))
        loads[g].start()

    barrier = pltpu.get_barrier_semaphore()
    for p in range(1, nx):
        signal(barrier, lax.rem(mx + p, nx), my)
    pl.when(has_low)(lambda: signal(barrier, mx, my - 1))
    pl.when(has_high)(lambda: signal(barrier, mx, my + 1))

    def clear(first, count):
        def body(x):
            for c in range(3):
                for h in range(2):
                    w[x, c, h, first : first + count, :] = jnp.zeros((count, HALF), F32)

        return lambda: over_rows(0, 12, body)

    clear(0, 6)()
    clear(74, 6)()
    pl.when(jnp.logical_not(has_low))(clear(6, 2))
    pl.when(jnp.logical_not(has_high))(clear(72, 2))
    acc[...] = jnp.zeros_like(acc)

    lane = lax.broadcasted_iota(jnp.int32, (8, HALF), 1)
    sub = lax.broadcasted_iota(jnp.int32, (8, HALF), 0)
    source = lax.broadcasted_iota(jnp.int32, (ZL, ZL), 0)
    target = lax.broadcasted_iota(jnp.int32, (ZL, ZL), 1)
    wanted = 2 * lax.rem(target, HALF) + lax.div(target, HALF)
    order[...] = jnp.where(source == wanted, 1.0, 0.0).astype(BF16)

    def split(row):
        cells = jnp.concatenate([nat[c, row - 2] for c in range(3)], axis=0)
        high = cells.astype(BF16)
        rest = cells - high.astype(F32)
        mid = rest.astype(BF16)
        low = (rest - mid.astype(F32)).astype(BF16)
        high, mid, low = (
            jnp.dot(part, order[...], preferred_element_type=F32) for part in (high, mid, low)
        )
        cells = high + (mid + low)
        for c in range(3):
            for h in range(2):
                w[row, c, h, 8 : 8 + YL, :] = cells[
                    YL * c : YL * c + YL, HALF * h : HALF * h + HALF
                ]

    def edge(src, dst, rows_from, rows_to, count, sems, to):
        return pltpu.make_async_remote_copy(
            src_ref=w.at[pl.ds(src[0], src[1]), :, :, rows_from : rows_from + count, :],
            dst_ref=w.at[pl.ds(dst[0], dst[1]), :, :, rows_to : rows_to + count, :],
            send_sem=sems[0],
            recv_sem=sems[1],
            device_id=to,
            device_id_type=MESH,
        )

    slow_src, slow_dst = 2 + 6 * core, 10 - 10 * core
    fast_src, fast_dst = 8 - 6 * core, 10 * core
    slow_copies = [
        edge(
            (slow_src, 2), (slow_dst, 2), 8 + lo, 8 + lo, hi - lo,
            (slow_send.at[c], slow_recv.at[c]), (slow, my),
        )
        for c, (lo, hi) in enumerate(zip(CUTS[:-1], CUTS[1:]))
    ]
    fast_copy = edge((fast_src, 2), (fast_dst, 2), 8, 8, YL, (fast_send, fast_recv), (fast, my))
    to_low = edge((2, 8), (2, 8), 8, 72, 2, (wall_send.at[0], wall_recv.at[0]), (mx, my - 1))
    to_high = edge((2, 8), (2, 8), 70, 6, 2, (wall_send.at[1], wall_recv.at[1]), (mx, my + 1))
    corners = [
        edge(rows[0], rows[1], r, r, 2, (corner_send.at[i], corner_recv.at[i]), (to, my))
        for i, (rows, to, r) in enumerate(
            (
                (((slow_src, 2), (slow_dst, 2)), slow, 6),
                (((slow_src, 2), (slow_dst, 2)), slow, 72),
                (((fast_src, 2), (fast_dst, 2)), fast, 6),
                (((fast_src, 2), (fast_dst, 2)), fast, 72),
            )
        )
    ]

    def spans(q, ks, products=(True, True)):
        for e in range(2):
            for k in ks:
                if products[0] == products[1]:
                    span_unit(w, zu, dz, zp, base(q) + e, k, products[0])
                else:
                    row = base(q) + (core if e else 1 - core)
                    span_unit(w, zu, dz, zp, row, k, products[e])

    def strains(q, ks):
        for e in range(2):
            for k in ks:
                strain_unit(w, zu, dz, zs, vf, dv, sr, base(q) - 1 + e, k)

    def sums(q, ks):
        for k in ks:
            sums_unit(zs, zp, vf, dv, acc, base(q) - 2, k)

    inner = range(1, 8)
    loads[0].wait()
    split(base(8))
    split(base(8) + 1)
    for g, q in ((1, 6), (2, 4), (3, 2)):
        loads[g].wait()
        spans(q + 2, inner)
        split(base(q))
        split(base(q) + 1)
    strains(7, inner)
    spans(2, inner)
    pl.semaphore_wait(
        barrier, nx - 1 + has_low.astype(jnp.int32) + has_high.astype(jnp.int32)
    )
    slow_copies[0].start()
    pl.when(has_low)(to_low.start)
    pl.when(has_high)(to_high.start)
    fast_copy.start()
    for copy in slow_copies[1:]:
        copy.start()

    strains(5, inner)
    sums(6, range(2, 7))
    strains(3, inner)
    fast_copy.wait_recv()
    sums(4, range(2, 7))
    spans(0, inner, (False, True))
    strains(1, inner)
    sums(2, range(2, 7))

    @pl.when(has_low)
    def _():
        to_high.wait_recv()
        corners[0].start()
        corners[2].start()

    @pl.when(has_high)
    def _():
        to_low.wait_recv()
        corners[1].start()
        corners[3].start()

    for q in (8, 6, 4, 2):
        spans(q, (0, 8))
    for q in (7, 5, 3):
        strains(q, (0, 8))
    pl.when(has_low)(corners[2].wait_recv)
    pl.when(has_high)(corners[3].wait_recv)
    sums(6, (0, 1, 7, 8))
    spans(0, (0, 8), (False, True))
    sums(4, (0, 1, 7, 8))
    strains(1, (0, 8))
    sums(2, (0, 1, 7, 8))

    done_strains = done_sums = 0
    for c, copy in enumerate(slow_copies):
        last = c == len(slow_copies) - 1
        copy.wait_recv()
        if c == 0:
            pl.when(has_low)(corners[0].wait_recv)
        if last:
            pl.when(has_high)(corners[1].wait_recv)
        ready_strains = 9 if last else (CUTS[c + 1] + 1) // 8
        ready_sums = 9 if last else ready_strains - 1
        spans(10, range(done_strains, ready_strains), (True, False))
        strains(9, range(done_strains, ready_strains))
        sums(8, range(done_sums, ready_sums))
        done_strains, done_sums = ready_strains, ready_sums

    packs = []
    for p in range(2):
        table = jnp.zeros((8, HALF), F32)
        for k in range(9):
            column = jnp.sum(acc[p, at(k), :], axis=1, keepdims=True)
            table = jnp.where(lane == k, column, table)
        spread = pltpu.roll(table, 0, 1, stride=16, stride_axis=0)
        packs.append(jnp.sum(spread, axis=0, keepdims=True))
    for p in range(2):
        msg[p : p + 1, :] = packs[p]
        gath[mx, p : p + 1, :] = packs[p]

    for p in range(1, nx):
        pltpu.make_async_remote_copy(
            src_ref=msg,
            dst_ref=gath.at[mx],
            send_sem=sum_send,
            recv_sem=sum_recv,
            device_id=(lax.rem(mx + p, nx), my),
            device_id_type=MESH,
        ).start()

    even_lane = lax.rem(lane, 2) == 0
    pick_low = lax.div(lane, 2)
    pick_high = pick_low + 64

    def join(x):
        for m in range(8):
            even = sr[x + 1, 0, 8 * m + 2 : 8 * m + 10, :]
            odd = sr[x + 1, 1, 8 * m + 2 : 8 * m + 10, :]
            for side, source in enumerate((pick_low, pick_high)):
                strength[x, at(m), HALF * side : HALF * side + HALF] = jnp.where(
                    even_lane,
                    jnp.take_along_axis(even, source, axis=1),
                    jnp.take_along_axis(odd, source, axis=1),
                )

    over_rows(0, XL, join, 2)

    everyone = pltpu.make_async_remote_copy(
        src_ref=gath.at[0 : nx - 1],
        dst_ref=gath.at[0 : nx - 1],
        send_sem=sum_send,
        recv_sem=sum_recv,
        device_id=(right, my),
        device_id_type=MESH,
    )
    everyone.wait_recv()
    terms = [gath[i] for i in range(nx)]
    while len(terms) > 1:
        terms = [a + b for a, b in zip(terms[::2], terms[1::2])]
    total = terms[0]
    raw = jnp.clip(0.5 * (total[0:1, :] / total[1:2, :]), 0.0, clip_high)
    raw = jnp.broadcast_to(raw, (8, HALF))
    below = jnp.where(lane < 16, pltpu.roll(raw, 17, 1), pltpu.roll(raw, 16, 1))
    above = jnp.where(lane >= 112, pltpu.roll(raw, 111, 1), pltpu.roll(raw, 112, 1))
    below = jnp.where(jnp.logical_and(lane == 32, jnp.logical_not(has_low)), raw, below)
    above = jnp.where(jnp.logical_and(lane == 24, jnp.logical_not(has_high)), raw, above)
    smooth = 0.25 * below + 0.5 * raw + 0.25 * above
    row = lane + 2
    line = jnp.take_along_axis(
        smooth, lax.rem(16 * lax.rem(row, 8) + lax.div(row, 8), HALF), axis=1
    )
    coefficient[...] = line[0:1, 0:YL]
    row = 8 * lane + sub + 2
    table = jnp.take_along_axis(
        smooth, lax.rem(16 * lax.rem(row, 8) + lax.div(row, 8), HALF), axis=1
    )
    columns = [jnp.broadcast_to(table[:, m : m + 1], (8, HALF)) for m in range(8)]

    def scale(x):
        for m in range(8):
            for side in range(2):
                part = (x, at(m), slice(HALF * side, HALF * side + HALF))
                viscosity[part] = strength[part] * columns[m]

    over_rows(0, XL, scale, 2)

    for copy in slow_copies:
        copy.wait_send()
    fast_copy.wait_send()

    @pl.when(has_low)
    def _():
        to_low.wait_send()
        corners[0].wait_send()
        corners[2].wait_send()

    @pl.when(has_high)
    def _():
        to_high.wait_send()
        corners[1].wait_send()
        corners[3].wait_send()

    everyone.wait_send()


def store_kernel(coefficient, viscosity, coefficient_out, viscosity_out, sems):
    copies = [
        pltpu.make_async_copy(viscosity, viscosity_out, sems.at[0]),
        pltpu.make_async_copy(coefficient, coefficient_out, sems.at[1]),
    ]
    for copy in copies:
        copy.start()
    for copy in copies:
        copy.wait()


def local(nx, ny, velocity):
    vmem = pl.BlockSpec(memory_space=pltpu.VMEM)
    dma = pltpu.SemaphoreType.DMA
    coefficient, viscosity = pl.pallas_call(
        functools.partial(main_kernel, nx, ny),
        out_shape=(
            pltpu.VMEM((1, YL), F32),
            pltpu.VMEM((XL, YL, ZL), F32),
        ),
        in_specs=[pl.BlockSpec(memory_space=pl.ANY)],
        out_specs=(vmem, vmem),
        scratch_shapes=[
            pltpu.VMEM((3, XL, YL, ZL), F32),
            pltpu.VMEM((12, 3, 2, 80, HALF), F32),
            pltpu.VMEM((12, 3, 2, 72, HALF), F32),
            pltpu.VMEM((10, 3, 2, 72, HALF), F32),
            pltpu.VMEM((10, 6, 2, 72, HALF), F32),
            pltpu.VMEM((10, 6, 2, 72, HALF), F32),
            pltpu.VMEM((10, 3, 2, 88, HALF), F32),
            pltpu.VMEM((10, 3, 2, 72, HALF), F32),
            pltpu.VMEM((10, 2, 72, HALF), F32),
            pltpu.VMEM((XL, YL, ZL), F32),
            pltpu.VMEM((2, 72, HALF), F32),
            pltpu.VMEM((2, HALF), F32),
            pltpu.VMEM((nx, 2, HALF), F32),
            pltpu.VMEM((ZL, ZL), BF16),
            dma((4,)),
            dma((CHUNKS,)),
            dma((CHUNKS,)),
            dma,
            dma,
            dma((2,)),
            dma((2,)),
            dma((4,)),
            dma((4,)),
            dma,
            dma,
        ],
        compiler_params=pltpu.CompilerParams(collective_id=0, has_side_effects=True),
        name="germano",
    )(velocity)
    anywhere = pl.BlockSpec(memory_space=pl.ANY)
    coefficient, viscosity = pl.pallas_call(
        store_kernel,
        out_shape=(
            jax.ShapeDtypeStruct((1, YL), F32),
            jax.ShapeDtypeStruct((XL, YL, ZL), F32),
        ),
        in_specs=[vmem, vmem],
        out_specs=(anywhere, anywhere),
        scratch_shapes=[dma((2,))],
        name="store",
    )(
        pltpu.with_memory_space_constraint(coefficient, pltpu.VMEM),
        pltpu.with_memory_space_constraint(viscosity, pltpu.VMEM),
    )
    return coefficient.reshape(YL), viscosity


def solution(mesh):
    nx, ny = mesh.shape["gx"], mesh.shape["gy"]
    return jax.shard_map(
        functools.partial(local, nx, ny),
        mesh=mesh,
        in_specs=(P(None, "gx", "gy", None),),
        out_specs=(P("gy"), P("gx", "gy", None)),
        check_vma=False,
    )
```

```python
import functools

import jax
import jax.numpy as jnp
from jax import lax
from jax.experimental import pallas as pl
from jax.experimental.pallas import tpu as pltpu
from jax.sharding import PartitionSpec as P

F32 = jnp.float32
BF16 = jnp.bfloat16
MESH = pl.DeviceIdType.MESH
XL = 8
YL = 64
ZL = 256
HALF = 128
CUTS = (0, 24, 48, 56, 64)
CHUNKS = len(CUTS) - 1
clip_high = 0.1
TINY = 1.2e-38
PAIRS = ((0, 0), (1, 1), (2, 2), (0, 1), (0, 2), (1, 2))


def shifted(even, odd):
    return pltpu.roll(odd, 1, 1), pltpu.roll(even, HALF - 1, 1)


def span_sum(even, odd, before, after):
    pair = even + odd
    return pair + (before + even), pair + (after + odd)


def at(k):
    return slice(8 * k, 8 * k + 8)


def span_unit(w, zu, dz, zp, xi, k, products):
    r = 6 + 8 * k
    even = [w[xi, c, 0, r : r + 8, :] for c in range(3)]
    odd = [w[xi, c, 1, r : r + 8, :] for c in range(3)]
    before, after = [None] * 3, [None] * 3
    for c in range(3):
        before[c], after[c] = shifted(even[c], odd[c])
    for c in range(3):
        both = span_sum(even[c], odd[c], before[c], after[c])
        zu[xi, c, 0, at(k), :], zu[xi, c, 1, at(k), :] = both
        if products:
            dz[xi - 1, c, 0, at(k), :] = odd[c] - before[c]
            dz[xi - 1, c, 1, at(k), :] = after[c] - even[c]
    if products:
        for p, (a, b) in enumerate(PAIRS):
            both = span_sum(
                even[a] * even[b], odd[a] * odd[b], before[a] * before[b], after[a] * after[b]
            )
            zp[xi - 1, p, 0, at(k), :], zp[xi - 1, p, 1, at(k), :] = both


def tensor(stream, wall, span):
    d0, d1, d2 = stream[0], wall[1], span[2]
    t01 = wall[0] + 0.25 * stream[1]
    t02 = span[0] + 0.5 * stream[2]
    t12 = span[1] + 2.0 * wall[2]
    square = t01 * t01 + 0.25 * (0.5 * (d0 * d0) + t02 * t02 + t12 * t12)
    square = square + (2.0 * (d1 * d1) + 0.5 * (d2 * d2))
    return (d0, d1, d2, t01, t02, t12), square * lax.rsqrt(jnp.maximum(square, TINY))


def strain_unit(w, zu, dz, zs, vf, sr, xi, k):
    r = 6 + 8 * k
    stress = [None] * 2
    for h in range(2):
        stream = [
            w[xi + 2, c, h, r : r + 8, :] - w[xi, c, h, r : r + 8, :] for c in range(3)
        ]
        wall = [
            w[xi + 1, c, h, r + 1 : r + 9, :] - w[xi + 1, c, h, r - 1 : r + 7, :]
            for c in range(3)
        ]
        span = [dz[xi, c, h, at(k), :] for c in range(3)]
        parts, mag = tensor(stream, wall, span)
        quarter, half = 0.25 * mag, 0.5 * mag
        factors = (quarter, mag, half, half, quarter, quarter)
        stress[h] = [factors[p] * parts[p] for p in range(6)]
        sr[xi, h, at(k), :] = mag
    for p in range(6):
        before, after = shifted(stress[0][p], stress[1][p])
        both = span_sum(stress[0][p], stress[1][p], before, after)
        zs[xi, p, 0, at(k), :], zs[xi, p, 1, at(k), :] = both
    for c in range(3):
        for h in range(2):
            mid = zu[xi + 1, c, h, at(k), :]
            line = (zu[xi, c, h, at(k), :] + mid) + (zu[xi + 2, c, h, at(k), :] + mid)
            vf[xi, c, h, 8 + 8 * k : 16 + 8 * k, :] = 0.25 * line


def sums_unit(zs, zp, vf, acc, xo, k):
    j = 8 + 8 * k
    num = den = None
    middles, spans = [], []
    for i in range(2):
        middle = [[vf[xo + 1 + i, c, h, j : j + 8, :] for h in range(2)] for c in range(3)]
        span = []
        for even, odd in middle:
            before, after = shifted(even, odd)
            span.append((odd - before, after - even))
        middles.append(middle)
        spans.append(span)
    for h in range(2):

        def lines(ref, p):
            rows = [ref[xo + i, p, h, at(k), :] for i in range(4)]
            pair = [rows[i] + rows[i + 1] for i in range(3)]
            return pair[0] + pair[1], pair[1] + pair[2]

        stress = [lines(zs, p) for p in range(6)]
        product = [lines(zp, p) for p in range(6)]
        for i in range(2):
            xi = xo + 1 + i
            stream = [
                vf[xi + 1, c, h, j : j + 8, :] - vf[xi - 1, c, h, j : j + 8, :] for c in range(3)
            ]
            wall = [
                vf[xi, c, h, j + 1 : j + 9, :] - vf[xi, c, h, j - 1 : j + 7, :]
                for c in range(3)
            ]
            span = [spans[i][c][h] for c in range(3)]
            middle = [middles[i][c][h] for c in range(3)]
            parts, mag = tensor(stream, wall, span)
            twice, four = 2.0 * mag, 4.0 * mag
            factors = (mag, four, twice, twice, mag, mag)
            mo = [stress[p][i] - factors[p] * parts[p] for p in range(6)]
            lo = [product[p][i] - middle[a] * middle[b] for p, (a, b) in enumerate(PAIRS)]
            third = (lo[0] + lo[1] + lo[2]) * (1.0 / 3.0)
            n_diag = (lo[0] - third) * mo[0] + (lo[1] - third) * mo[1] + (lo[2] - third) * mo[2]
            n_off = lo[3] * mo[3] + lo[4] * mo[4] + lo[5] * mo[5]
            d_diag = mo[0] * mo[0] + mo[1] * mo[1] + mo[2] * mo[2]
            d_off = mo[3] * mo[3] + mo[4] * mo[4] + mo[5] * mo[5]
            n = n_diag + (n_off + n_off)
            d = d_diag + (d_off + d_off)
            num = n if num is None else num + n
            den = d if den is None else den + d
    acc[0, at(k), :] += num
    acc[1, at(k), :] += den


def over_rows(base, count, body, each=1):
    def step(i, carry):
        for e in range(each):
            body(base + each * i + e)
        return carry

    if count == each:
        step(0, 0)
    else:
        lax.fori_loop(0, count // each, step, 0)


def main_kernel(
    nx, ny,
    vel, coefficient, viscosity,
    nat, w, zu, dz, zp, zs, vf, sr, strength, acc, msg, gath, order,
    in_sem, slow_send, slow_recv, fast_send, fast_recv, wall_send, wall_recv,
    corner_send, corner_recv, sum_send, sum_recv,
):
    mx = lax.axis_index("gx")
    my = lax.axis_index("gy")
    core = lax.rem(mx, 2)
    right = lax.rem(mx + 1, nx)
    left = lax.rem(mx + nx - 1, nx)
    slow = core * right + (1 - core) * left
    fast = core * left + (1 - core) * right
    has_low = my > 0
    has_high = my < ny - 1

    def base(q):
        return core * q + (1 - core) * (10 - q)

    def peers(far_first):
        if nx != 32:
            return [lax.rem(mx + p, nx) for p in range(1, nx)]
        px, pz = mx // 8, lax.rem(mx, 8) // 2
        xs = [lax.rem(px + d, 4) * 8 for d in range(4)]
        zs_ = [lax.rem(pz + d, 4) * 2 for d in range(4)]
        steps = [(a, b, c) for a in range(4) for b in range(4) for c in range(2)][1:]
        steps.sort(key=lambda t: min(t[0], 4 - t[0]) + min(t[1], 4 - t[1]), reverse=far_first)
        return [xs[a] + (zs_[b] + (1 - core if c else core)) for a, b, c in steps]

    def signal(sem, x, y):
        pl.semaphore_signal(sem, inc=1, device_id=(x, y), device_id_type=MESH)

    barrier = pltpu.get_barrier_semaphore()
    loads = []
    for g, q in enumerate((8, 6, 4, 2)):
        cells = pl.ds(base(q) - 2, 2)
        loads.append(pltpu.make_async_copy(vel.at[:, cells], nat.at[:, cells], in_sem.at[g]))
        if g == 0:
            loads[g].start()
    for peer in peers(True):
        signal(barrier, peer, my)
    pl.when(has_low)(lambda: signal(barrier, mx, my - 1))
    pl.when(has_high)(lambda: signal(barrier, mx, my + 1))
    for load in loads[1:]:
        load.start()

    def clear(first, count):
        def body(x):
            for c in range(3):
                for h in range(2):
                    w[x, c, h, first : first + count, :] = jnp.zeros((count, HALF), F32)

        return lambda: over_rows(0, 12, body)

    clear(0, 6)()
    clear(74, 6)()
    pl.when(jnp.logical_not(has_low))(clear(6, 2))
    pl.when(jnp.logical_not(has_high))(clear(72, 2))
    acc[...] = jnp.zeros_like(acc)

    lane = lax.broadcasted_iota(jnp.int32, (8, HALF), 1)
    sub = lax.broadcasted_iota(jnp.int32, (8, HALF), 0)
    source = lax.broadcasted_iota(jnp.int32, (ZL, ZL), 0)
    target = lax.broadcasted_iota(jnp.int32, (ZL, ZL), 1)
    wanted = 2 * lax.rem(target, HALF) + lax.div(target, HALF)
    order[...] = jnp.where(source == wanted, 1.0, 0.0).astype(BF16)

    def split(row, lo=0, hi=YL):
        rows = hi - lo
        cells = jnp.concatenate([nat[c, row - 2, lo:hi, :] for c in range(3)], axis=0)
        high = cells.astype(BF16)
        rest = cells - high.astype(F32)
        mid = rest.astype(BF16)
        low = (rest - mid.astype(F32)).astype(BF16)
        high, mid, low = (
            jnp.dot(part, order[...], preferred_element_type=F32) for part in (high, mid, low)
        )
        cells = high + (mid + low)
        for c in range(3):
            for h in range(2):
                w[row, c, h, 8 + lo : 8 + hi, :] = cells[
                    rows * c : rows * c + rows, HALF * h : HALF * h + HALF
                ]

    def edge(src, dst, rows_from, rows_to, count, sems, to):
        return pltpu.make_async_remote_copy(
            src_ref=w.at[pl.ds(src[0], src[1]), :, :, rows_from : rows_from + count, :],
            dst_ref=w.at[pl.ds(dst[0], dst[1]), :, :, rows_to : rows_to + count, :],
            send_sem=sems[0],
            recv_sem=sems[1],
            device_id=to,
            device_id_type=MESH,
        )

    slow_src, slow_dst = 2 + 6 * core, 10 - 10 * core
    fast_src, fast_dst = 8 - 6 * core, 10 * core
    slow_copies = [
        edge(
            (slow_src, 2), (slow_dst, 2), 8 + lo, 8 + lo, hi - lo,
            (slow_send.at[c], slow_recv.at[c]), (slow, my),
        )
        for c, (lo, hi) in enumerate(zip(CUTS[:-1], CUTS[1:]))
    ]
    fast_copy = edge((fast_src, 2), (fast_dst, 2), 8, 8, YL, (fast_send, fast_recv), (fast, my))
    to_low = edge((2, 8), (2, 8), 8, 72, 2, (wall_send.at[0], wall_recv.at[0]), (mx, my - 1))
    to_high = edge((2, 8), (2, 8), 70, 6, 2, (wall_send.at[1], wall_recv.at[1]), (mx, my + 1))
    corners = [
        edge(rows[0], rows[1], r, r, 2, (corner_send.at[i], corner_recv.at[i]), (to, my))
        for i, (rows, to, r) in enumerate(
            (
                (((slow_src, 2), (slow_dst, 2)), slow, 6),
                (((slow_src, 2), (slow_dst, 2)), slow, 72),
                (((fast_src, 2), (fast_dst, 2)), fast, 6),
                (((fast_src, 2), (fast_dst, 2)), fast, 72),
            )
        )
    ]

    def spans(q, ks, products=(True, True)):
        for e in range(2):
            for k in ks:
                if products[0] == products[1]:
                    span_unit(w, zu, dz, zp, base(q) + e, k, products[0])
                else:
                    row = base(q) + (core if e else 1 - core)
                    span_unit(w, zu, dz, zp, row, k, products[e])

    def strains(q, ks):
        for e in range(2):
            for k in ks:
                strain_unit(w, zu, dz, zs, vf, sr, base(q) - 1 + e, k)

    def sums(q, ks):
        for k in ks:
            sums_unit(zs, zp, vf, acc, base(q) - 2, k)

    inner = range(1, 8)
    px, pz = mx // 8, lax.rem(mx, 8) // 2
    either, both = jnp.logical_or, jnp.logical_and
    first = either(pz == 0, both(pz == 1, px < 2))
    second = either(
        both(pz == 1, px >= 2), either(both(pz == 2, px < 2), both(pz == 3, px == 0))
    )
    third = jnp.logical_not(either(first, second))

    def meet():
        pl.semaphore_wait(
            barrier, nx - 1 + has_low.astype(jnp.int32) + has_high.astype(jnp.int32)
        )
        for copy in slow_copies:
            copy.start()

    def send_near():
        pl.when(has_low)(to_low.start)
        pl.when(has_high)(to_high.start)
        fast_copy.start()

    loads[0].wait()
    split(base(8))
    split(base(8) + 1)
    pl.when(third)(meet)
    for g, q in ((1, 6), (2, 4), (3, 2)):
        loads[g].wait()
        spans(q + 2, inner)
        split(base(q))
        split(base(q) + 1)
    pl.when(third)(send_near)
    strains(7, inner)
    spans(2, inner)

    @pl.when(second)
    def _():
        meet()
        send_near()

    strains(5, inner)
    sums(6, range(2, 7))
    strains(3, inner)

    @pl.when(first)
    def _():
        meet()
        send_near()

    fast_copy.wait_recv()
    sums(4, range(2, 7))
    spans(0, inner, (False, True))
    strains(1, inner)
    sums(2, range(2, 7))

    @pl.when(has_low)
    def _():
        to_high.wait_recv()
        corners[0].start()
        corners[2].start()

    @pl.when(has_high)
    def _():
        to_low.wait_recv()
        corners[1].start()
        corners[3].start()

    for q in (8, 6, 4, 2):
        spans(q, (0, 8))
    for q in (7, 5, 3):
        strains(q, (0, 8))
    pl.when(has_low)(corners[2].wait_recv)
    pl.when(has_high)(corners[3].wait_recv)
    sums(6, (0, 1, 7, 8))
    spans(0, (0, 8), (False, True))
    sums(4, (0, 1, 7, 8))
    strains(1, (0, 8))
    sums(2, (0, 1, 7, 8))

    done_strains = done_sums = 0
    for c, copy in enumerate(slow_copies):
        last = c == len(slow_copies) - 1
        copy.wait_recv()
        if c == 0:
            pl.when(has_low)(corners[0].wait_recv)
        if last:
            pl.when(has_high)(corners[1].wait_recv)
        ready_strains = 9 if last else (CUTS[c + 1] + 1) // 8
        ready_sums = 9 if last else ready_strains - 1
        spans(10, range(done_strains, ready_strains), (True, False))
        strains(9, range(done_strains, ready_strains))
        sums(8, range(done_sums, ready_sums))
        done_strains, done_sums = ready_strains, ready_sums

    packs = []
    for p in range(2):
        table = jnp.zeros((8, HALF), F32)
        for k in range(9):
            column = jnp.sum(acc[p, at(k), :], axis=1, keepdims=True)
            table = jnp.where(lane == k, column, table)
        spread = pltpu.roll(table, 0, 1, stride=16, stride_axis=0)
        packs.append(jnp.sum(spread, axis=0, keepdims=True))
    for p in range(2):
        msg[p : p + 1, :] = packs[p]
        gath[mx, p : p + 1, :] = packs[p]

    for peer in peers(True):
        pltpu.make_async_remote_copy(
            src_ref=msg,
            dst_ref=gath.at[mx],
            send_sem=sum_send,
            recv_sem=sum_recv,
            device_id=(peer, my),
            device_id_type=MESH,
        ).start()

    even_lane = lax.rem(lane, 2) == 0
    pick_low = lax.div(lane, 2)
    pick_high = pick_low + 64

    def join(x):
        for m in range(8):
            even = sr[x + 1, 0, 8 * m + 2 : 8 * m + 10, :]
            odd = sr[x + 1, 1, 8 * m + 2 : 8 * m + 10, :]
            for side, source in enumerate((pick_low, pick_high)):
                strength[x, at(m), HALF * side : HALF * side + HALF] = jnp.where(
                    even_lane,
                    jnp.take_along_axis(even, source, axis=1),
                    jnp.take_along_axis(odd, source, axis=1),
                )

    over_rows(0, XL, join, 2)

    everyone = pltpu.make_async_remote_copy(
        src_ref=gath.at[0 : nx - 1],
        dst_ref=gath.at[0 : nx - 1],
        send_sem=sum_send,
        recv_sem=sum_recv,
        device_id=(right, my),
        device_id_type=MESH,
    )
    everyone.wait_recv()
    terms = [gath[i] for i in range(nx)]
    while len(terms) > 1:
        terms = [a + b for a, b in zip(terms[::2], terms[1::2])]
    total = terms[0]
    raw = jnp.clip(0.5 * (total[0:1, :] / total[1:2, :]), 0.0, clip_high)
    raw = jnp.broadcast_to(raw, (8, HALF))
    below = jnp.where(lane < 16, pltpu.roll(raw, 17, 1), pltpu.roll(raw, 16, 1))
    above = jnp.where(lane >= 112, pltpu.roll(raw, 111, 1), pltpu.roll(raw, 112, 1))
    below = jnp.where(jnp.logical_and(lane == 32, jnp.logical_not(has_low)), raw, below)
    above = jnp.where(jnp.logical_and(lane == 24, jnp.logical_not(has_high)), raw, above)
    smooth = 0.25 * below + 0.5 * raw + 0.25 * above
    row = lane + 2
    line = jnp.take_along_axis(
        smooth, lax.rem(16 * lax.rem(row, 8) + lax.div(row, 8), HALF), axis=1
    )
    coefficient[...] = line[0:1, 0:YL]
    row = 8 * lane + sub + 2
    table = jnp.take_along_axis(
        smooth, lax.rem(16 * lax.rem(row, 8) + lax.div(row, 8), HALF), axis=1
    )
    columns = [jnp.broadcast_to(table[:, m : m + 1], (8, HALF)) for m in range(8)]

    def scale(x):
        for m in range(8):
            for side in range(2):
                part = (x, at(m), slice(HALF * side, HALF * side + HALF))
                viscosity[part] = strength[part] * columns[m]

    over_rows(0, XL, scale, 2)

    for copy in slow_copies:
        copy.wait_send()
    fast_copy.wait_send()

    @pl.when(has_low)
    def _():
        to_low.wait_send()
        corners[0].wait_send()
        corners[2].wait_send()

    @pl.when(has_high)
    def _():
        to_high.wait_send()
        corners[1].wait_send()
        corners[3].wait_send()

    everyone.wait_send()


def store_kernel(coefficient, viscosity, coefficient_out, viscosity_out, sems):
    copies = [
        pltpu.make_async_copy(viscosity, viscosity_out, sems.at[0]),
        pltpu.make_async_copy(coefficient, coefficient_out, sems.at[1]),
    ]
    for copy in copies:
        copy.start()
    for copy in copies:
        copy.wait()


def local(nx, ny, velocity):
    vmem = pl.BlockSpec(memory_space=pltpu.VMEM)
    dma = pltpu.SemaphoreType.DMA
    coefficient, viscosity = pl.pallas_call(
        functools.partial(main_kernel, nx, ny),
        out_shape=(
            pltpu.VMEM((1, YL), F32),
            pltpu.VMEM((XL, YL, ZL), F32),
        ),
        in_specs=[pl.BlockSpec(memory_space=pl.ANY)],
        out_specs=(vmem, vmem),
        scratch_shapes=[
            pltpu.VMEM((3, XL, YL, ZL), F32),
            pltpu.VMEM((12, 3, 2, 80, HALF), F32),
            pltpu.VMEM((12, 3, 2, 72, HALF), F32),
            pltpu.VMEM((10, 3, 2, 72, HALF), F32),
            pltpu.VMEM((10, 6, 2, 72, HALF), F32),
            pltpu.VMEM((10, 6, 2, 72, HALF), F32),
            pltpu.VMEM((10, 3, 2, 88, HALF), F32),
            pltpu.VMEM((10, 2, 72, HALF), F32),
            pltpu.VMEM((XL, YL, ZL), F32),
            pltpu.VMEM((2, 72, HALF), F32),
            pltpu.VMEM((2, HALF), F32),
            pltpu.VMEM((nx, 2, HALF), F32),
            pltpu.VMEM((ZL, ZL), BF16),
            dma((4,)),
            dma((CHUNKS,)),
            dma((CHUNKS,)),
            dma,
            dma,
            dma((2,)),
            dma((2,)),
            dma((4,)),
            dma((4,)),
            dma,
            dma,
        ],
        compiler_params=pltpu.CompilerParams(collective_id=0, has_side_effects=True),
        name="germano",
    )(velocity)
    anywhere = pl.BlockSpec(memory_space=pl.ANY)
    coefficient, viscosity = pl.pallas_call(
        store_kernel,
        out_shape=(
            jax.ShapeDtypeStruct((1, YL), F32),
            jax.ShapeDtypeStruct((XL, YL, ZL), F32),
        ),
        in_specs=[vmem, vmem],
        out_specs=(anywhere, anywhere),
        scratch_shapes=[dma((2,))],
        name="store",
    )(
        pltpu.with_memory_space_constraint(coefficient, pltpu.VMEM),
        pltpu.with_memory_space_constraint(viscosity, pltpu.VMEM),
    )
    return coefficient.reshape(YL), viscosity


def solution(mesh):
    nx, ny = mesh.shape["gx"], mesh.shape["gy"]
    return jax.shard_map(
        functools.partial(local, nx, ny),
        mesh=mesh,
        in_specs=(P(None, "gx", "gy", None),),
        out_specs=(P("gy"), P("gx", "gy", None)),
        check_vma=False,
    )
```

```python
import functools

import jax
import jax.numpy as jnp
from jax import lax
from jax.experimental import pallas as pl
from jax.experimental.pallas import tpu as pltpu
from jax.sharding import PartitionSpec as P

F32 = jnp.float32
BF16 = jnp.bfloat16
MESH = pl.DeviceIdType.MESH
XL = 8
YL = 64
ZL = 256
HALF = 128
NEAR = (1, -1, 2, -2, 8, -8)
FAR = (8, -8, 16)
CUTS = (0, 24, 48, 56, 64)
CHUNKS = len(CUTS) - 1
clip_high = 0.1
TINY = 1.2e-38
PAIRS = ((0, 0), (1, 1), (2, 2), (0, 1), (0, 2), (1, 2))


def shifted(even, odd):
    return pltpu.roll(odd, 1, 1), pltpu.roll(even, HALF - 1, 1)


def span_sum(even, odd, before, after):
    pair = even + odd
    return pair + (before + even), pair + (after + odd)


def at(k):
    return slice(8 * k, 8 * k + 8)


def span_unit(w, zu, dz, zp, xi, k, products):
    r = 6 + 8 * k
    even = [w[xi, c, 0, r : r + 8, :] for c in range(3)]
    odd = [w[xi, c, 1, r : r + 8, :] for c in range(3)]
    before, after = [None] * 3, [None] * 3
    for c in range(3):
        before[c], after[c] = shifted(even[c], odd[c])
    for c in range(3):
        both = span_sum(even[c], odd[c], before[c], after[c])
        zu[xi, c, 0, at(k), :], zu[xi, c, 1, at(k), :] = both
        if products:
            dz[xi - 1, c, 0, at(k), :] = odd[c] - before[c]
            dz[xi - 1, c, 1, at(k), :] = after[c] - even[c]
    if products:
        for p, (a, b) in enumerate(PAIRS):
            both = span_sum(
                even[a] * even[b], odd[a] * odd[b], before[a] * before[b], after[a] * after[b]
            )
            zp[xi - 1, p, 0, at(k), :], zp[xi - 1, p, 1, at(k), :] = both


def tensor(stream, wall, span):
    d0, d1, d2 = stream[0], wall[1], span[2]
    t01 = wall[0] + 0.25 * stream[1]
    t02 = span[0] + 0.5 * stream[2]
    t12 = span[1] + 2.0 * wall[2]
    square = t01 * t01 + 0.25 * (0.5 * (d0 * d0) + t02 * t02 + t12 * t12)
    square = square + (2.0 * (d1 * d1) + 0.5 * (d2 * d2))
    return (d0, d1, d2, t01, t02, t12), square * lax.rsqrt(jnp.maximum(square, TINY))


def strain_unit(w, zu, dz, zs, vf, sr, xi, k):
    r = 6 + 8 * k
    stress = [None] * 2
    for h in range(2):
        stream = [
            w[xi + 2, c, h, r : r + 8, :] - w[xi, c, h, r : r + 8, :] for c in range(3)
        ]
        wall = [
            w[xi + 1, c, h, r + 1 : r + 9, :] - w[xi + 1, c, h, r - 1 : r + 7, :]
            for c in range(3)
        ]
        span = [dz[xi, c, h, at(k), :] for c in range(3)]
        parts, mag = tensor(stream, wall, span)
        quarter, half = 0.25 * mag, 0.5 * mag
        factors = (quarter, mag, half, half, quarter, quarter)
        stress[h] = [factors[p] * parts[p] for p in range(6)]
        sr[xi, h, at(k), :] = mag
    for p in range(6):
        before, after = shifted(stress[0][p], stress[1][p])
        both = span_sum(stress[0][p], stress[1][p], before, after)
        zs[xi, p, 0, at(k), :], zs[xi, p, 1, at(k), :] = both
    for c in range(3):
        for h in range(2):
            mid = zu[xi + 1, c, h, at(k), :]
            line = (zu[xi, c, h, at(k), :] + mid) + (zu[xi + 2, c, h, at(k), :] + mid)
            vf[xi, c, h, 8 + 8 * k : 16 + 8 * k, :] = 0.25 * line


def sums_unit(zs, zp, vf, acc, xo, k):
    j = 8 + 8 * k
    num = den = None
    middles, spans = [], []
    for i in range(2):
        middle = [[vf[xo + 1 + i, c, h, j : j + 8, :] for h in range(2)] for c in range(3)]
        span = []
        for even, odd in middle:
            before, after = shifted(even, odd)
            span.append((odd - before, after - even))
        middles.append(middle)
        spans.append(span)
    for h in range(2):

        def lines(ref, p):
            rows = [ref[xo + i, p, h, at(k), :] for i in range(4)]
            pair = [rows[i] + rows[i + 1] for i in range(3)]
            return pair[0] + pair[1], pair[1] + pair[2]

        stress = [lines(zs, p) for p in range(6)]
        product = [lines(zp, p) for p in range(6)]
        for i in range(2):
            xi = xo + 1 + i
            stream = [
                vf[xi + 1, c, h, j : j + 8, :] - vf[xi - 1, c, h, j : j + 8, :] for c in range(3)
            ]
            wall = [
                vf[xi, c, h, j + 1 : j + 9, :] - vf[xi, c, h, j - 1 : j + 7, :]
                for c in range(3)
            ]
            span = [spans[i][c][h] for c in range(3)]
            middle = [middles[i][c][h] for c in range(3)]
            parts, mag = tensor(stream, wall, span)
            twice, four = 2.0 * mag, 4.0 * mag
            factors = (mag, four, twice, twice, mag, mag)
            mo = [stress[p][i] - factors[p] * parts[p] for p in range(6)]
            lo = [product[p][i] - middle[a] * middle[b] for p, (a, b) in enumerate(PAIRS)]
            third = (lo[0] + lo[1] + lo[2]) * (1.0 / 3.0)
            n_diag = (lo[0] - third) * mo[0] + (lo[1] - third) * mo[1] + (lo[2] - third) * mo[2]
            n_off = lo[3] * mo[3] + lo[4] * mo[4] + lo[5] * mo[5]
            d_diag = mo[0] * mo[0] + mo[1] * mo[1] + mo[2] * mo[2]
            d_off = mo[3] * mo[3] + mo[4] * mo[4] + mo[5] * mo[5]
            n = n_diag + (n_off + n_off)
            d = d_diag + (d_off + d_off)
            num = n if num is None else num + n
            den = d if den is None else den + d
    acc[0, at(k), :] += num
    acc[1, at(k), :] += den


def over_rows(base, count, body, each=1):
    def step(i, carry):
        for e in range(each):
            body(base + each * i + e)
        return carry

    if count == each:
        step(0, 0)
    else:
        lax.fori_loop(0, count // each, step, 0)


def main_kernel(
    nx, ny,
    vel, coefficient, viscosity,
    nat, w, zu, dz, zp, zs, vf, sr, strength, acc, msg, gath, order,
    in_sem, slow_send, slow_recv, fast_send, fast_recv, wall_send, wall_recv,
    corner_send, corner_recv, sum_send, sum_recv, round_sem,
):
    mx = lax.axis_index("gx")
    my = lax.axis_index("gy")
    core = lax.rem(mx, 2)
    right = lax.rem(mx + 1, nx)
    left = lax.rem(mx + nx - 1, nx)
    slow = core * right + (1 - core) * left
    fast = core * left + (1 - core) * right
    has_low = my > 0
    has_high = my < ny - 1

    def base(q):
        return core * q + (1 - core) * (10 - q)

    def peers(far_first):
        if nx != 32:
            return [lax.rem(mx + p, nx) for p in range(1, nx)]
        px, pz = mx // 8, lax.rem(mx, 8) // 2
        xs = [lax.rem(px + d, 4) * 8 for d in range(4)]
        zs_ = [lax.rem(pz + d, 4) * 2 for d in range(4)]
        steps = [(a, b, c) for a in range(4) for b in range(4) for c in range(2)][1:]
        steps.sort(key=lambda t: min(t[0], 4 - t[0]) + min(t[1], 4 - t[1]), reverse=far_first)
        return [xs[a] + (zs_[b] + (1 - core if c else core)) for a, b, c in steps]

    def signal(sem, x, y):
        pl.semaphore_signal(sem, inc=1, device_id=(x, y), device_id_type=MESH)

    def along(step):
        return lax.rem(mx + (step + nx), nx)

    barrier = pltpu.get_barrier_semaphore()
    for step in NEAR:
        signal(barrier, along(step), my)
    pl.when(has_low)(lambda: signal(barrier, mx, my - 1))
    pl.when(has_high)(lambda: signal(barrier, mx, my + 1))
    loads = []
    for g, q in enumerate((8, 6, 4, 2)):
        cells = pl.ds(base(q) - 2, 2)
        loads.append(pltpu.make_async_copy(vel.at[:, cells], nat.at[:, cells], in_sem.at[g]))
        loads[g].start()

    def clear(first, count):
        def body(x):
            for c in range(3):
                for h in range(2):
                    w[x, c, h, first : first + count, :] = jnp.zeros((count, HALF), F32)

        return lambda: over_rows(0, 12, body)

    clear(0, 6)()
    clear(74, 6)()
    pl.when(jnp.logical_not(has_low))(clear(6, 2))
    pl.when(jnp.logical_not(has_high))(clear(72, 2))
    acc[...] = jnp.zeros_like(acc)

    lane = lax.broadcasted_iota(jnp.int32, (8, HALF), 1)
    sub = lax.broadcasted_iota(jnp.int32, (8, HALF), 0)
    source = lax.broadcasted_iota(jnp.int32, (ZL, ZL), 0)
    target = lax.broadcasted_iota(jnp.int32, (ZL, ZL), 1)
    wanted = 2 * lax.rem(target, HALF) + lax.div(target, HALF)
    order[...] = jnp.where(source == wanted, 1.0, 0.0).astype(BF16)

    def split(row, lo=0, hi=YL):
        rows = hi - lo
        cells = jnp.concatenate([nat[c, row - 2, lo:hi, :] for c in range(3)], axis=0)
        high = cells.astype(BF16)
        rest = cells - high.astype(F32)
        mid = rest.astype(BF16)
        low = (rest - mid.astype(F32)).astype(BF16)
        high, mid, low = (
            jnp.dot(part, order[...], preferred_element_type=F32) for part in (high, mid, low)
        )
        cells = high + (mid + low)
        for c in range(3):
            for h in range(2):
                w[row, c, h, 8 + lo : 8 + hi, :] = cells[
                    rows * c : rows * c + rows, HALF * h : HALF * h + HALF
                ]

    def edge(src, dst, rows_from, rows_to, count, sems, to):
        return pltpu.make_async_remote_copy(
            src_ref=w.at[pl.ds(src[0], src[1]), :, :, rows_from : rows_from + count, :],
            dst_ref=w.at[pl.ds(dst[0], dst[1]), :, :, rows_to : rows_to + count, :],
            send_sem=sems[0],
            recv_sem=sems[1],
            device_id=to,
            device_id_type=MESH,
        )

    slow_src, slow_dst = 2 + 6 * core, 10 - 10 * core
    fast_src, fast_dst = 8 - 6 * core, 10 * core
    slow_copies = [
        edge(
            (slow_src, 2), (slow_dst, 2), 8 + lo, 8 + lo, hi - lo,
            (slow_send.at[c], slow_recv.at[c]), (slow, my),
        )
        for c, (lo, hi) in enumerate(zip(CUTS[:-1], CUTS[1:]))
    ]
    fast_copy = edge((fast_src, 2), (fast_dst, 2), 8, 8, YL, (fast_send, fast_recv), (fast, my))
    to_low = edge((2, 8), (2, 8), 8, 72, 2, (wall_send.at[0], wall_recv.at[0]), (mx, my - 1))
    to_high = edge((2, 8), (2, 8), 70, 6, 2, (wall_send.at[1], wall_recv.at[1]), (mx, my + 1))
    corners = [
        edge(rows[0], rows[1], r, r, 2, (corner_send.at[i], corner_recv.at[i]), (to, my))
        for i, (rows, to, r) in enumerate(
            (
                (((slow_src, 2), (slow_dst, 2)), slow, 6),
                (((slow_src, 2), (slow_dst, 2)), slow, 72),
                (((fast_src, 2), (fast_dst, 2)), fast, 6),
                (((fast_src, 2), (fast_dst, 2)), fast, 72),
            )
        )
    ]

    def spans(q, ks, products=(True, True)):
        for e in range(2):
            for k in ks:
                if products[0] == products[1]:
                    span_unit(w, zu, dz, zp, base(q) + e, k, products[0])
                else:
                    row = base(q) + (core if e else 1 - core)
                    span_unit(w, zu, dz, zp, row, k, products[e])

    def strains(q, ks):
        for e in range(2):
            for k in ks:
                strain_unit(w, zu, dz, zs, vf, sr, base(q) - 1 + e, k)

    def sums(q, ks):
        for k in ks:
            sums_unit(zs, zp, vf, acc, base(q) - 2, k)

    inner = range(1, 8)
    px, pz = mx // 8, lax.rem(mx, 8) // 2
    either, both = jnp.logical_or, jnp.logical_and
    first = pz == 0
    second = both(px == 0, pz > 0)
    third = jnp.logical_not(either(first, second))

    def meet():
        pl.semaphore_wait(
            barrier, len(NEAR) + has_low.astype(jnp.int32) + has_high.astype(jnp.int32)
        )
        for copy in slow_copies:
            copy.start()
        for step in NEAR:
            signal(round_sem.at[0], along(step), my)

    def send_near():
        pl.when(has_low)(to_low.start)
        pl.when(has_high)(to_high.start)
        fast_copy.start()

    loads[0].wait()
    split(base(8))
    split(base(8) + 1)
    pl.when(third)(meet)
    for g, q in ((1, 6), (2, 4), (3, 2)):
        loads[g].wait()
        spans(q + 2, inner)
        split(base(q))
        split(base(q) + 1)
    pl.when(third)(send_near)
    strains(7, inner)
    spans(2, inner)

    @pl.when(second)
    def _():
        meet()
        send_near()

    strains(5, inner)
    sums(6, range(2, 7))
    strains(3, inner)

    @pl.when(first)
    def _():
        meet()
        send_near()

    fast_copy.wait_recv()
    sums(4, range(2, 7))
    spans(0, inner, (False, True))
    strains(1, inner)
    sums(2, range(2, 7))

    pl.semaphore_wait(round_sem.at[0], len(NEAR))
    for step in FAR:
        signal(round_sem.at[1], along(step), my)

    @pl.when(has_low)
    def _():
        to_high.wait_recv()
        corners[0].start()
        corners[2].start()

    @pl.when(has_high)
    def _():
        to_low.wait_recv()
        corners[1].start()
        corners[3].start()

    for q in (8, 6, 4, 2):
        spans(q, (0, 8))
    for q in (7, 5, 3):
        strains(q, (0, 8))
    pl.when(has_low)(corners[2].wait_recv)
    pl.when(has_high)(corners[3].wait_recv)
    sums(6, (0, 1, 7, 8))
    spans(0, (0, 8), (False, True))
    sums(4, (0, 1, 7, 8))
    strains(1, (0, 8))
    sums(2, (0, 1, 7, 8))

    done_strains = done_sums = 0
    for c, copy in enumerate(slow_copies):
        last = c == len(slow_copies) - 1
        copy.wait_recv()
        if c == 0:
            pl.when(has_low)(corners[0].wait_recv)
        if last:
            pl.when(has_high)(corners[1].wait_recv)
        ready_strains = 9 if last else (CUTS[c + 1] + 1) // 8
        ready_sums = 9 if last else ready_strains - 1
        spans(10, range(done_strains, ready_strains), (True, False))
        strains(9, range(done_strains, ready_strains))
        sums(8, range(done_sums, ready_sums))
        done_strains, done_sums = ready_strains, ready_sums

    packs = []
    for p in range(2):
        table = jnp.zeros((8, HALF), F32)
        for k in range(9):
            column = jnp.sum(acc[p, at(k), :], axis=1, keepdims=True)
            table = jnp.where(lane == k, column, table)
        spread = pltpu.roll(table, 0, 1, stride=16, stride_axis=0)
        packs.append(jnp.sum(spread, axis=0, keepdims=True))
    for p in range(2):
        msg[p : p + 1, :] = packs[p]
        gath[mx, p : p + 1, :] = packs[p]

    pl.semaphore_wait(round_sem.at[1], len(FAR))
    for peer in peers(True):
        pltpu.make_async_remote_copy(
            src_ref=msg,
            dst_ref=gath.at[mx],
            send_sem=sum_send,
            recv_sem=sum_recv,
            device_id=(peer, my),
            device_id_type=MESH,
        ).start()

    even_lane = lax.rem(lane, 2) == 0
    pick_low = lax.div(lane, 2)
    pick_high = pick_low + 64

    def join(x):
        for m in range(8):
            even = sr[x + 1, 0, 8 * m + 2 : 8 * m + 10, :]
            odd = sr[x + 1, 1, 8 * m + 2 : 8 * m + 10, :]
            for side, source in enumerate((pick_low, pick_high)):
                strength[x, at(m), HALF * side : HALF * side + HALF] = jnp.where(
                    even_lane,
                    jnp.take_along_axis(even, source, axis=1),
                    jnp.take_along_axis(odd, source, axis=1),
                )

    over_rows(0, XL, join, 2)

    everyone = pltpu.make_async_remote_copy(
        src_ref=gath.at[0 : nx - 1],
        dst_ref=gath.at[0 : nx - 1],
        send_sem=sum_send,
        recv_sem=sum_recv,
        device_id=(right, my),
        device_id_type=MESH,
    )
    everyone.wait_recv()
    terms = [gath[i] for i in range(nx)]
    while len(terms) > 1:
        terms = [a + b for a, b in zip(terms[::2], terms[1::2])]
    total = terms[0]
    raw = jnp.clip(0.5 * (total[0:1, :] / total[1:2, :]), 0.0, clip_high)
    raw = jnp.broadcast_to(raw, (8, HALF))
    below = jnp.where(lane < 16, pltpu.roll(raw, 17, 1), pltpu.roll(raw, 16, 1))
    above = jnp.where(lane >= 112, pltpu.roll(raw, 111, 1), pltpu.roll(raw, 112, 1))
    below = jnp.where(jnp.logical_and(lane == 32, jnp.logical_not(has_low)), raw, below)
    above = jnp.where(jnp.logical_and(lane == 24, jnp.logical_not(has_high)), raw, above)
    smooth = 0.25 * below + 0.5 * raw + 0.25 * above
    row = lane + 2
    line = jnp.take_along_axis(
        smooth, lax.rem(16 * lax.rem(row, 8) + lax.div(row, 8), HALF), axis=1
    )
    coefficient[...] = line[0:1, 0:YL]
    row = 8 * lane + sub + 2
    table = jnp.take_along_axis(
        smooth, lax.rem(16 * lax.rem(row, 8) + lax.div(row, 8), HALF), axis=1
    )
    columns = [jnp.broadcast_to(table[:, m : m + 1], (8, HALF)) for m in range(8)]

    def scale(x):
        for m in range(8):
            for side in range(2):
                part = (x, at(m), slice(HALF * side, HALF * side + HALF))
                viscosity[part] = strength[part] * columns[m]

    over_rows(0, XL, scale, 2)

    for copy in slow_copies:
        copy.wait_send()
    fast_copy.wait_send()

    @pl.when(has_low)
    def _():
        to_low.wait_send()
        corners[0].wait_send()
        corners[2].wait_send()

    @pl.when(has_high)
    def _():
        to_high.wait_send()
        corners[1].wait_send()
        corners[3].wait_send()

    everyone.wait_send()


def store_kernel(coefficient, viscosity, coefficient_out, viscosity_out, sems):
    copies = [
        pltpu.make_async_copy(viscosity, viscosity_out, sems.at[0]),
        pltpu.make_async_copy(coefficient, coefficient_out, sems.at[1]),
    ]
    for copy in copies:
        copy.start()
    for copy in copies:
        copy.wait()


def local(nx, ny, velocity):
    vmem = pl.BlockSpec(memory_space=pltpu.VMEM)
    dma = pltpu.SemaphoreType.DMA
    coefficient, viscosity = pl.pallas_call(
        functools.partial(main_kernel, nx, ny),
        out_shape=(
            pltpu.VMEM((1, YL), F32),
            pltpu.VMEM((XL, YL, ZL), F32),
        ),
        in_specs=[pl.BlockSpec(memory_space=pl.ANY)],
        out_specs=(vmem, vmem),
        scratch_shapes=[
            pltpu.VMEM((3, XL, YL, ZL), F32),
            pltpu.VMEM((12, 3, 2, 80, HALF), F32),
            pltpu.VMEM((12, 3, 2, 72, HALF), F32),
            pltpu.VMEM((10, 3, 2, 72, HALF), F32),
            pltpu.VMEM((10, 6, 2, 72, HALF), F32),
            pltpu.VMEM((10, 6, 2, 72, HALF), F32),
            pltpu.VMEM((10, 3, 2, 88, HALF), F32),
            pltpu.VMEM((10, 2, 72, HALF), F32),
            pltpu.VMEM((XL, YL, ZL), F32),
            pltpu.VMEM((2, 72, HALF), F32),
            pltpu.VMEM((2, HALF), F32),
            pltpu.VMEM((nx, 2, HALF), F32),
            pltpu.VMEM((ZL, ZL), BF16),
            dma((4,)),
            dma((CHUNKS,)),
            dma((CHUNKS,)),
            dma,
            dma,
            dma((2,)),
            dma((2,)),
            dma((4,)),
            dma((4,)),
            dma,
            dma,
            pltpu.SemaphoreType.REGULAR((2,)),
        ],
        compiler_params=pltpu.CompilerParams(collective_id=0, has_side_effects=True),
        name="germano",
    )(velocity)
    anywhere = pl.BlockSpec(memory_space=pl.ANY)
    coefficient, viscosity = pl.pallas_call(
        store_kernel,
        out_shape=(
            jax.ShapeDtypeStruct((1, YL), F32),
            jax.ShapeDtypeStruct((XL, YL, ZL), F32),
        ),
        in_specs=[vmem, vmem],
        out_specs=(anywhere, anywhere),
        scratch_shapes=[dma((2,))],
        name="store",
    )(
        pltpu.with_memory_space_constraint(coefficient, pltpu.VMEM),
        pltpu.with_memory_space_constraint(viscosity, pltpu.VMEM),
    )
    return coefficient.reshape(YL), viscosity


def solution(mesh):
    nx, ny = mesh.shape["gx"], mesh.shape["gy"]
    return jax.shard_map(
        functools.partial(local, nx, ny),
        mesh=mesh,
        in_specs=(P(None, "gx", "gy", None),),
        out_specs=(P("gy"), P("gx", "gy", None)),
        check_vma=False,
    )
```

```python
import functools

import jax
import jax.numpy as jnp
from jax import lax
from jax.experimental import pallas as pl
from jax.experimental.pallas import tpu as pltpu
from jax.sharding import PartitionSpec as P

F32 = jnp.float32
BF16 = jnp.bfloat16
MESH = pl.DeviceIdType.MESH
XL = 8
YL = 64
ZL = 256
HALF = 128
NEAR = (1, -1, 2, -2, 8, -8)
FAR = (8, -8, 16)
CUTS = (0, 24, 48, 56, 64)
CHUNKS = len(CUTS) - 1
clip_high = 0.1
TINY = 1.2e-38
PAIRS = ((0, 0), (1, 1), (2, 2), (0, 1), (0, 2), (1, 2))


def shifted(even, odd):
    return pltpu.roll(odd, 1, 1), pltpu.roll(even, HALF - 1, 1)


def span_sum(even, odd, before, after):
    pair = even + odd
    return pair + (before + even), pair + (after + odd)


def at(k):
    return slice(8 * k, 8 * k + 8)


def span_unit(w, zu, dz, zp, xi, k, products):
    r = 6 + 8 * k
    even = [w[xi, c, 0, r : r + 8, :] for c in range(3)]
    odd = [w[xi, c, 1, r : r + 8, :] for c in range(3)]
    before, after = [None] * 3, [None] * 3
    for c in range(3):
        before[c], after[c] = shifted(even[c], odd[c])
    for c in range(3):
        both = span_sum(even[c], odd[c], before[c], after[c])
        zu[xi, c, 0, at(k), :], zu[xi, c, 1, at(k), :] = both
        if products:
            dz[xi - 1, c, 0, at(k), :] = odd[c] - before[c]
            dz[xi - 1, c, 1, at(k), :] = after[c] - even[c]
    if products:
        for p, (a, b) in enumerate(PAIRS):
            both = span_sum(
                even[a] * even[b], odd[a] * odd[b], before[a] * before[b], after[a] * after[b]
            )
            zp[xi - 1, p, 0, at(k), :], zp[xi - 1, p, 1, at(k), :] = both


def tensor(stream, wall, span):
    d0, d1, d2 = stream[0], wall[1], span[2]
    t01 = wall[0] + 0.25 * stream[1]
    t02 = span[0] + 0.5 * stream[2]
    t12 = span[1] + 2.0 * wall[2]
    square = t01 * t01 + 0.25 * (0.5 * (d0 * d0) + t02 * t02 + t12 * t12)
    square = square + (2.0 * (d1 * d1) + 0.5 * (d2 * d2))
    return (d0, d1, d2, t01, t02, t12), square * lax.rsqrt(jnp.maximum(square, TINY))


def strain_unit(w, zu, dz, zs, vf, sr, xi, k):
    r = 6 + 8 * k
    stress = [None] * 2
    for h in range(2):
        stream = [
            w[xi + 2, c, h, r : r + 8, :] - w[xi, c, h, r : r + 8, :] for c in range(3)
        ]
        wall = [
            w[xi + 1, c, h, r + 1 : r + 9, :] - w[xi + 1, c, h, r - 1 : r + 7, :]
            for c in range(3)
        ]
        span = [dz[xi, c, h, at(k), :] for c in range(3)]
        parts, mag = tensor(stream, wall, span)
        quarter, half = 0.25 * mag, 0.5 * mag
        factors = (quarter, mag, half, half, quarter, quarter)
        stress[h] = [factors[p] * parts[p] for p in range(6)]
        sr[xi, h, at(k), :] = mag
    for p in range(6):
        before, after = shifted(stress[0][p], stress[1][p])
        both = span_sum(stress[0][p], stress[1][p], before, after)
        zs[xi, p, 0, at(k), :], zs[xi, p, 1, at(k), :] = both
    for c in range(3):
        for h in range(2):
            mid = zu[xi + 1, c, h, at(k), :]
            line = (zu[xi, c, h, at(k), :] + mid) + (zu[xi + 2, c, h, at(k), :] + mid)
            vf[xi, c, h, 8 + 8 * k : 16 + 8 * k, :] = 0.25 * line


def sums_unit(zs, zp, vf, acc, xo, k):
    j = 8 + 8 * k
    num = den = None
    middles, spans = [], []
    for i in range(2):
        middle = [[vf[xo + 1 + i, c, h, j : j + 8, :] for h in range(2)] for c in range(3)]
        span = []
        for even, odd in middle:
            before, after = shifted(even, odd)
            span.append((odd - before, after - even))
        middles.append(middle)
        spans.append(span)
    for h in range(2):

        def lines(ref, p):
            rows = [ref[xo + i, p, h, at(k), :] for i in range(4)]
            pair = [rows[i] + rows[i + 1] for i in range(3)]
            return pair[0] + pair[1], pair[1] + pair[2]

        stress = [lines(zs, p) for p in range(6)]
        product = [lines(zp, p) for p in range(6)]
        for i in range(2):
            xi = xo + 1 + i
            stream = [
                vf[xi + 1, c, h, j : j + 8, :] - vf[xi - 1, c, h, j : j + 8, :] for c in range(3)
            ]
            wall = [
                vf[xi, c, h, j + 1 : j + 9, :] - vf[xi, c, h, j - 1 : j + 7, :]
                for c in range(3)
            ]
            span = [spans[i][c][h] for c in range(3)]
            middle = [middles[i][c][h] for c in range(3)]
            parts, mag = tensor(stream, wall, span)
            twice, four = 2.0 * mag, 4.0 * mag
            factors = (mag, four, twice, twice, mag, mag)
            mo = [stress[p][i] - factors[p] * parts[p] for p in range(6)]
            lo = [product[p][i] - middle[a] * middle[b] for p, (a, b) in enumerate(PAIRS)]
            third = (lo[0] + lo[1] + lo[2]) * (1.0 / 3.0)
            n_diag = (lo[0] - third) * mo[0] + (lo[1] - third) * mo[1] + (lo[2] - third) * mo[2]
            n_off = lo[3] * mo[3] + lo[4] * mo[4] + lo[5] * mo[5]
            d_diag = mo[0] * mo[0] + mo[1] * mo[1] + mo[2] * mo[2]
            d_off = mo[3] * mo[3] + mo[4] * mo[4] + mo[5] * mo[5]
            n = n_diag + (n_off + n_off)
            d = d_diag + (d_off + d_off)
            num = n if num is None else num + n
            den = d if den is None else den + d
    acc[0, at(k), :] += num
    acc[1, at(k), :] += den


def over_rows(base, count, body, each=1):
    def step(i, carry):
        for e in range(each):
            body(base + each * i + e)
        return carry

    if count == each:
        step(0, 0)
    else:
        lax.fori_loop(0, count // each, step, 0)


def main_kernel(
    nx, ny,
    vel, coefficient, viscosity,
    nat, w, zu, dz, zp, zs, vf, sr, strength, acc, msg, gath, order,
    in_sem, slow_send, slow_recv, fast_send, fast_recv, wall_send, wall_recv,
    corner_send, corner_recv, sum_send, sum_recv, round_sem,
):
    mx = lax.axis_index("gx")
    my = lax.axis_index("gy")
    core = lax.rem(mx, 2)
    right = lax.rem(mx + 1, nx)
    left = lax.rem(mx + nx - 1, nx)
    slow = core * right + (1 - core) * left
    fast = core * left + (1 - core) * right
    has_low = my > 0
    has_high = my < ny - 1

    def base(q):
        return core * q + (1 - core) * (10 - q)

    def peers(far_first):
        if nx != 32:
            return [lax.rem(mx + p, nx) for p in range(1, nx)]
        px, pz = mx // 8, lax.rem(mx, 8) // 2
        xs = [lax.rem(px + d, 4) * 8 for d in range(4)]
        zs_ = [lax.rem(pz + d, 4) * 2 for d in range(4)]
        steps = [(a, b, c) for a in range(4) for b in range(4) for c in range(2)][1:]
        steps.sort(key=lambda t: min(t[0], 4 - t[0]) + min(t[1], 4 - t[1]), reverse=far_first)
        return [xs[a] + (zs_[b] + (1 - core if c else core)) for a, b, c in steps]

    def signal(sem, x, y):
        pl.semaphore_signal(sem, inc=1, device_id=(x, y), device_id_type=MESH)

    def along(step):
        return lax.rem(mx + (step + nx), nx)

    barrier = pltpu.get_barrier_semaphore()
    for step in NEAR:
        signal(barrier, along(step), my)
    pl.when(has_low)(lambda: signal(barrier, mx, my - 1))
    pl.when(has_high)(lambda: signal(barrier, mx, my + 1))
    loads = []
    for g, q in enumerate((8, 6, 4, 2)):
        cells = pl.ds(base(q) - 2, 2)
        loads.append(pltpu.make_async_copy(vel.at[:, cells], nat.at[:, cells], in_sem.at[g]))
        loads[g].start()

    def clear(first, count):
        def body(x):
            for c in range(3):
                for h in range(2):
                    w[x, c, h, first : first + count, :] = jnp.zeros((count, HALF), F32)

        return lambda: over_rows(0, 12, body)

    clear(0, 6)()
    clear(74, 6)()
    pl.when(jnp.logical_not(has_low))(clear(6, 2))
    pl.when(jnp.logical_not(has_high))(clear(72, 2))
    acc[...] = jnp.zeros_like(acc)

    lane = lax.broadcasted_iota(jnp.int32, (8, HALF), 1)
    sub = lax.broadcasted_iota(jnp.int32, (8, HALF), 0)
    source = lax.broadcasted_iota(jnp.int32, (ZL, ZL), 0)
    target = lax.broadcasted_iota(jnp.int32, (ZL, ZL), 1)
    wanted = 2 * lax.rem(target, HALF) + lax.div(target, HALF)
    order[...] = jnp.where(source == wanted, 1.0, 0.0).astype(BF16)

    def split(row, lo=0, hi=YL):
        rows = hi - lo
        cells = jnp.concatenate([nat[c, row - 2, lo:hi, :] for c in range(3)], axis=0)
        high = cells.astype(BF16)
        rest = cells - high.astype(F32)
        mid = rest.astype(BF16)
        low = (rest - mid.astype(F32)).astype(BF16)
        high, mid, low = (
            jnp.dot(part, order[...], preferred_element_type=F32) for part in (high, mid, low)
        )
        cells = high + (mid + low)
        for c in range(3):
            for h in range(2):
                w[row, c, h, 8 + lo : 8 + hi, :] = cells[
                    rows * c : rows * c + rows, HALF * h : HALF * h + HALF
                ]

    def edge(src, dst, rows_from, rows_to, count, sems, to):
        return pltpu.make_async_remote_copy(
            src_ref=w.at[pl.ds(src[0], src[1]), :, :, rows_from : rows_from + count, :],
            dst_ref=w.at[pl.ds(dst[0], dst[1]), :, :, rows_to : rows_to + count, :],
            send_sem=sems[0],
            recv_sem=sems[1],
            device_id=to,
            device_id_type=MESH,
        )

    slow_src, slow_dst = 2 + 6 * core, 10 - 10 * core
    fast_src, fast_dst = 8 - 6 * core, 10 * core
    slow_copies = [
        edge(
            (slow_src, 2), (slow_dst, 2), 8 + lo, 8 + lo, hi - lo,
            (slow_send.at[c], slow_recv.at[c]), (slow, my),
        )
        for c, (lo, hi) in enumerate(zip(CUTS[:-1], CUTS[1:]))
    ]
    fast_copy = edge((fast_src, 2), (fast_dst, 2), 8, 8, YL, (fast_send, fast_recv), (fast, my))
    to_low = edge((2, 8), (2, 8), 8, 72, 2, (wall_send.at[0], wall_recv.at[0]), (mx, my - 1))
    to_high = edge((2, 8), (2, 8), 70, 6, 2, (wall_send.at[1], wall_recv.at[1]), (mx, my + 1))
    corners = [
        edge(rows[0], rows[1], r, r, 2, (corner_send.at[i], corner_recv.at[i]), (to, my))
        for i, (rows, to, r) in enumerate(
            (
                (((slow_src, 2), (slow_dst, 2)), slow, 6),
                (((slow_src, 2), (slow_dst, 2)), slow, 72),
                (((fast_src, 2), (fast_dst, 2)), fast, 6),
                (((fast_src, 2), (fast_dst, 2)), fast, 72),
            )
        )
    ]

    def spans(q, ks, products=(True, True)):
        for e in range(2):
            for k in ks:
                if products[0] == products[1]:
                    span_unit(w, zu, dz, zp, base(q) + e, k, products[0])
                else:
                    row = base(q) + (core if e else 1 - core)
                    span_unit(w, zu, dz, zp, row, k, products[e])

    def strains(q, ks):
        for e in range(2):
            for k in ks:
                strain_unit(w, zu, dz, zs, vf, sr, base(q) - 1 + e, k)

    def sums(q, ks):
        for k in ks:
            sums_unit(zs, zp, vf, acc, base(q) - 2, k)

    inner = range(1, 8)
    px, pz = mx // 8, lax.rem(mx, 8) // 2
    either, both = jnp.logical_or, jnp.logical_and
    first = pz == 0
    second = both(px == 0, pz > 0)
    third = jnp.logical_not(either(first, second))

    def meet():
        pl.semaphore_wait(
            barrier, len(NEAR) + has_low.astype(jnp.int32) + has_high.astype(jnp.int32)
        )
        for copy in slow_copies:
            copy.start()
        for step in NEAR:
            signal(round_sem.at[0], along(step), my)

    def send_near():
        pl.when(has_low)(to_low.start)
        pl.when(has_high)(to_high.start)
        fast_copy.start()

    loads[0].wait()
    split(base(8))
    split(base(8) + 1)
    pl.when(third)(meet)
    for g, q in ((1, 6), (2, 4), (3, 2)):
        loads[g].wait()
        spans(q + 2, inner)
        split(base(q))
        split(base(q) + 1)
    pl.when(third)(send_near)
    strains(7, inner)
    spans(2, inner)

    @pl.when(second)
    def _():
        meet()
        send_near()

    strains(5, inner)
    sums(6, range(2, 7))
    strains(3, inner)

    @pl.when(first)
    def _():
        meet()
        send_near()

    fast_copy.wait_recv()
    sums(4, range(2, 7))
    spans(0, inner, (False, True))
    strains(1, inner)
    sums(2, range(2, 7))

    pl.semaphore_wait(round_sem.at[0], len(NEAR))
    for step in FAR:
        signal(round_sem.at[1], along(step), my)

    @pl.when(has_low)
    def _():
        to_high.wait_recv()
        corners[0].start()
        corners[2].start()

    @pl.when(has_high)
    def _():
        to_low.wait_recv()
        corners[1].start()
        corners[3].start()

    for q in (8, 6, 4, 2):
        spans(q, (0, 8))
    for q in (7, 5, 3):
        strains(q, (0, 8))
    pl.when(has_low)(corners[2].wait_recv)
    pl.when(has_high)(corners[3].wait_recv)
    sums(6, (0, 1, 7, 8))
    spans(0, (0, 8), (False, True))
    sums(4, (0, 1, 7, 8))
    strains(1, (0, 8))
    sums(2, (0, 1, 7, 8))

    done_strains, done_sums = 1, 2
    for c, copy in enumerate(slow_copies):
        copy.wait_recv()
        ready_strains = (CUTS[c + 1] + 1) // 8
        spans(10, range(done_strains, ready_strains), (True, False))
        strains(9, range(done_strains, ready_strains))
        sums(8, range(done_sums, ready_strains - 1))
        done_strains, done_sums = ready_strains, ready_strains - 1
    pl.when(has_low)(corners[0].wait_recv)
    pl.when(has_high)(corners[1].wait_recv)
    spans(10, (0, 8), (True, False))
    strains(9, (0, 8))
    sums(8, (0, 1, 7, 8))

    packs = []
    for p in range(2):
        table = jnp.zeros((8, HALF), F32)
        for k in range(9):
            column = jnp.sum(acc[p, at(k), :], axis=1, keepdims=True)
            table = jnp.where(lane == k, column, table)
        spread = pltpu.roll(table, 0, 1, stride=16, stride_axis=0)
        packs.append(jnp.sum(spread, axis=0, keepdims=True))
    for p in range(2):
        msg[p : p + 1, :] = packs[p]
        gath[mx, p : p + 1, :] = packs[p]

    pl.semaphore_wait(round_sem.at[1], len(FAR))
    for peer in peers(True):
        pltpu.make_async_remote_copy(
            src_ref=msg,
            dst_ref=gath.at[mx],
            send_sem=sum_send,
            recv_sem=sum_recv,
            device_id=(peer, my),
            device_id_type=MESH,
        ).start()

    even_lane = lax.rem(lane, 2) == 0
    pick_low = lax.div(lane, 2)
    pick_high = pick_low + 64

    def join(x):
        for m in range(8):
            even = sr[x + 1, 0, 8 * m + 2 : 8 * m + 10, :]
            odd = sr[x + 1, 1, 8 * m + 2 : 8 * m + 10, :]
            for side, source in enumerate((pick_low, pick_high)):
                strength[x, at(m), HALF * side : HALF * side + HALF] = jnp.where(
                    even_lane,
                    jnp.take_along_axis(even, source, axis=1),
                    jnp.take_along_axis(odd, source, axis=1),
                )

    over_rows(0, XL, join, 2)

    everyone = pltpu.make_async_remote_copy(
        src_ref=gath.at[0 : nx - 1],
        dst_ref=gath.at[0 : nx - 1],
        send_sem=sum_send,
        recv_sem=sum_recv,
        device_id=(right, my),
        device_id_type=MESH,
    )
    everyone.wait_recv()
    terms = [gath[i] for i in range(nx)]
    while len(terms) > 1:
        terms = [a + b for a, b in zip(terms[::2], terms[1::2])]
    total = terms[0]
    raw = jnp.clip(0.5 * (total[0:1, :] / total[1:2, :]), 0.0, clip_high)
    raw = jnp.broadcast_to(raw, (8, HALF))
    below = jnp.where(lane < 16, pltpu.roll(raw, 17, 1), pltpu.roll(raw, 16, 1))
    above = jnp.where(lane >= 112, pltpu.roll(raw, 111, 1), pltpu.roll(raw, 112, 1))
    below = jnp.where(jnp.logical_and(lane == 32, jnp.logical_not(has_low)), raw, below)
    above = jnp.where(jnp.logical_and(lane == 24, jnp.logical_not(has_high)), raw, above)
    smooth = 0.25 * below + 0.5 * raw + 0.25 * above
    row = lane + 2
    line = jnp.take_along_axis(
        smooth, lax.rem(16 * lax.rem(row, 8) + lax.div(row, 8), HALF), axis=1
    )
    coefficient[...] = line[0:1, 0:YL]
    row = 8 * lane + sub + 2
    table = jnp.take_along_axis(
        smooth, lax.rem(16 * lax.rem(row, 8) + lax.div(row, 8), HALF), axis=1
    )
    columns = [jnp.broadcast_to(table[:, m : m + 1], (8, HALF)) for m in range(8)]

    def scale(x):
        for m in range(8):
            for side in range(2):
                part = (x, at(m), slice(HALF * side, HALF * side + HALF))
                viscosity[part] = strength[part] * columns[m]

    over_rows(0, XL, scale, 2)

    for copy in slow_copies:
        copy.wait_send()
    fast_copy.wait_send()

    @pl.when(has_low)
    def _():
        to_low.wait_send()
        corners[0].wait_send()
        corners[2].wait_send()

    @pl.when(has_high)
    def _():
        to_high.wait_send()
        corners[1].wait_send()
        corners[3].wait_send()

    everyone.wait_send()


def store_kernel(coefficient, viscosity, coefficient_out, viscosity_out, sems):
    copies = [
        pltpu.make_async_copy(viscosity, viscosity_out, sems.at[0]),
        pltpu.make_async_copy(coefficient, coefficient_out, sems.at[1]),
    ]
    for copy in copies:
        copy.start()
    for copy in copies:
        copy.wait()


def local(nx, ny, velocity):
    vmem = pl.BlockSpec(memory_space=pltpu.VMEM)
    dma = pltpu.SemaphoreType.DMA
    coefficient, viscosity = pl.pallas_call(
        functools.partial(main_kernel, nx, ny),
        out_shape=(
            pltpu.VMEM((1, YL), F32),
            pltpu.VMEM((XL, YL, ZL), F32),
        ),
        in_specs=[pl.BlockSpec(memory_space=pl.ANY)],
        out_specs=(vmem, vmem),
        scratch_shapes=[
            pltpu.VMEM((3, XL, YL, ZL), F32),
            pltpu.VMEM((12, 3, 2, 80, HALF), F32),
            pltpu.VMEM((12, 3, 2, 72, HALF), F32),
            pltpu.VMEM((10, 3, 2, 72, HALF), F32),
            pltpu.VMEM((10, 6, 2, 72, HALF), F32),
            pltpu.VMEM((10, 6, 2, 72, HALF), F32),
            pltpu.VMEM((10, 3, 2, 88, HALF), F32),
            pltpu.VMEM((10, 2, 72, HALF), F32),
            pltpu.VMEM((XL, YL, ZL), F32),
            pltpu.VMEM((2, 72, HALF), F32),
            pltpu.VMEM((2, HALF), F32),
            pltpu.VMEM((nx, 2, HALF), F32),
            pltpu.VMEM((ZL, ZL), BF16),
            dma((4,)),
            dma((CHUNKS,)),
            dma((CHUNKS,)),
            dma,
            dma,
            dma((2,)),
            dma((2,)),
            dma((4,)),
            dma((4,)),
            dma,
            dma,
            pltpu.SemaphoreType.REGULAR((2,)),
        ],
        compiler_params=pltpu.CompilerParams(collective_id=0, has_side_effects=True),
        name="germano",
    )(velocity)
    anywhere = pl.BlockSpec(memory_space=pl.ANY)
    coefficient, viscosity = pl.pallas_call(
        store_kernel,
        out_shape=(
            jax.ShapeDtypeStruct((1, YL), F32),
            jax.ShapeDtypeStruct((XL, YL, ZL), F32),
        ),
        in_specs=[vmem, vmem],
        out_specs=(anywhere, anywhere),
        scratch_shapes=[dma((2,))],
        name="store",
    )(
        pltpu.with_memory_space_constraint(coefficient, pltpu.VMEM),
        pltpu.with_memory_space_constraint(viscosity, pltpu.VMEM),
    )
    return coefficient.reshape(YL), viscosity


def solution(mesh):
    nx, ny = mesh.shape["gx"], mesh.shape["gy"]
    return jax.shard_map(
        functools.partial(local, nx, ny),
        mesh=mesh,
        in_specs=(P(None, "gx", "gy", None),),
        out_specs=(P("gy"), P("gx", "gy", None)),
        check_vma=False,
    )
```
